32 devices in a mesh: movie: 16 (over z, y, x), user: 2 (over core).
Axes of the slice: x: 2, y: 2, z: 4, core: 2. Of those that a mesh axis runs over, the one named last changes fastest.
Arguments:
- movie_ids: int32 [128, 128], P(('movie', 'user')), may hold values from 0 to 17919, as said below
- ratings: int32 [128, 128], P(('movie', 'user')), may hold values from 0 to 4
- valid: int32 [128, 128], P(('movie', 'user')), may hold values from 0 to 1, as said below
- weights: bfloat16 [5, 17920, 1024], P(None, 'movie'), may hold values from -0.5 to 0.5
- vis_bias: float32 [5, 17920], P(None, 'movie'), may hold values from -5 to 260
- hid_bias: float32 [1024], replicated, may hold values from -5 to 5
Outputs:
- weight_grad: float32 [5, 17920, 1024], P(None, 'movie')
- visible_grad: float32 [5, 17920], P(None, 'movie')
- hidden_grad: float32 [1024], replicated
- positive_hidden: float32 [128, 1024], P(('movie', 'user'))
The draws below stay inside these ranges and needn't reach their ends.
Inputs may be any that keep to these rules, and one draw needn't show every extreme that they name: `movie_ids`: movie ids within one user's block are distinct. Of the slots with valid 1 among the users of one device (4 consecutive users), at most 96 name movies of any one block of 1120 consecutive movie ids; in every draw some such block takes exactly 96 from the users of every device. Slots with valid 0 are padding and count nowhere.
All inputs are finite; a program needn't handle non-finite values.
Results may differ from the reference program's by a relative error of at most 0.0054.
Values may be sent and summed in bfloat16 or wider, within the bound.
No kernel may reach another device: no remote copies, remote signals or barrier semaphores. Data moves between devices by JAX's collectives and lax.ppermute only.
A program may use at most 128 MiB of HBM per device.

```python
import math
import jax
import jax.numpy as jnp
from jax import lax

F = 1024
LEVELS = 5
MOVIES = 17920
SLOTS = 128
USR_DEV = 4
OWNERS = 16
MOV_DEV = 1120
USERS = 128
CAP = 96


def rating_layout(key):
    base_key = jax.random.fold_in(key, 7101)
    busiest = jax.random.randint(jax.random.fold_in(base_key, 1), (), 0, OWNERS)
    device_slots = USR_DEV * SLOTS
    position = jnp.arange(device_slots, dtype=jnp.int32)
    listed = jnp.where(position < CAP, busiest, (busiest + 1 + (position - CAP) % (OWNERS - 1)) % OWNERS)
    devices = USERS // USR_DEV
    device_keys = jax.random.split(jax.random.fold_in(base_key, 2), devices)
    shuffle = jax.vmap(lambda single: jax.random.permutation(single, device_slots))(device_keys)
    owner_ids = listed[shuffle].reshape(USERS, SLOTS).astype(jnp.int32)
    offsets_table = jax.random.randint(jax.random.fold_in(base_key, 3), (USERS, OWNERS), 0, MOV_DEV)
    matching = owner_ids[:, :, None] == owner_ids[:, None, :]
    slot_index = jnp.arange(SLOTS, dtype=jnp.int32)
    earlier = slot_index[None, :] < slot_index[:, None]
    occurrence = jnp.sum((matching & earlier[None]).astype(jnp.int32), axis=2)
    offset = jnp.take_along_axis(offsets_table, owner_ids, axis=1)
    local_index = (offset + occurrence) % MOV_DEV
    movie_block = (owner_ids * MOV_DEV + local_index).astype(jnp.int32)
    coin_flip = jax.random.randint(jax.random.fold_in(base_key, 4), (USERS, SLOTS), 0, 4)
    usable = jnp.where(owner_ids == busiest, 1, jnp.where(coin_flip > 0, 1, 0)).astype(jnp.int32)
    return (movie_block, usable)


def draw_movie_ids(key, part):
    return rating_layout(key)[0]


def draw_valid(key, part):
    return rating_layout(key)[1]


def draw_vis_bias(key, part):
    baseline = jnp.clip(jax.random.normal(jax.random.fold_in(key, 11), (LEVELS, MOVIES), jnp.float32), -4.0, 4.0)
    return baseline.astype(jnp.float32)


def plant(result, own_key, least, top_value):
    longest = result.shape.index(max(result.shape))
    spots = []
    for shift in (0, 1):
        where = [jax.random.randint(jax.random.fold_in(own_key, axis), (), 0, length) for axis, length in enumerate(result.shape)]
        where[longest] = (where[longest] + shift) % result.shape[longest]
        spots.append(tuple(where))
    return result.at[spots[0]].set(least).at[spots[1]].set(top_value)


def block_scale(key, extent, pieces, smallest, high):
    def one(axis_at, parts):
        steps = jax.random.uniform(jax.random.fold_in(jax.random.fold_in(key, 6), axis_at), (parts,), jnp.float32, smallest / len(pieces), high / len(pieces))
        return jnp.repeat(jnp.exp(steps), extent[axis_at] // parts).reshape((-1,) + (1,) * (len(extent) - axis_at - 1))

    level = one(*pieces[0])
    for cut in pieces[1:]:
        level = level * one(*cut)
    return level


def normal_values(stream_key, shape, scale, most, cuts=(), kind=jnp.bfloat16):
    drawn = scale * jax.random.normal(stream_key, shape, jnp.float32)
    if cuts:
        drawn = drawn * block_scale(stream_key, shape, cuts, -0.22, 0.18)
    return jnp.clip(drawn, -most, most).astype(kind)


def setup_inputs(seed: int = 0) -> dict:
    streams_of = jax.random.split(jax.random.key(seed), 7)
    movie_ids = draw_movie_ids(jax.random.fold_in(streams_of[6], 71), 0)
    ratings = plant(jax.random.randint(streams_of[1], (USERS, SLOTS), 0, LEVELS), jax.random.fold_in(streams_of[1], 1), 0, LEVELS - 1).astype(jnp.int32)
    valid = draw_valid(jax.random.fold_in(streams_of[6], 71), 0)
    weights = normal_values(streams_of[3], (LEVELS, MOVIES, F), SLOTS ** -0.5, 0.5, ((1, 16),))
    vis_bias = draw_vis_bias(jax.random.fold_in(streams_of[6], 71), 0)
    hid_bias = normal_values(streams_of[5], (F,), 1.0, 5.0, (), jnp.float32)
    return {"movie_ids": movie_ids, "ratings": ratings, "valid": valid, "weights": weights, "vis_bias": vis_bias, "hid_bias": hid_bias}


def reference(movie_ids, ratings, valid, weights, vis_bias, hid_bias):
    user_count, slot_count = movie_ids.shape
    levels, movies, hidden = weights.shape
    block_size = math.gcd(user_count, 16)
    block_count = user_count // block_size
    rating_levels = jnp.arange(levels, dtype=jnp.int32)
    highest_rating = lax.Precision.HIGHEST

    def advance(totals, block_index):
        weight_grad, visible_grad, hidden_grad = totals
        first_row = (block_index * block_size).astype(jnp.int32)
        movie_block = lax.dynamic_slice_in_dim(movie_ids, first_row, block_size, 0)
        rating_block = lax.dynamic_slice_in_dim(ratings, first_row, block_size, 0)
        usable = lax.dynamic_slice_in_dim(valid, first_row, block_size, 0).astype(jnp.float32)
        movie_weight_rows = weights[:, movie_block].astype(jnp.float32)
        visible_bias_rows = vis_bias[:, movie_block]
        observed_mask = (rating_block[None] == rating_levels[:, None, None]).astype(jnp.float32) * usable[None]
        positive_statistics = jnp.einsum("drp,drpv->rv", observed_mask, movie_weight_rows, precision=highest_rating)
        hidden_pos = jax.nn.sigmoid(hid_bias[None, :] + positive_statistics)
        positive_lower_part = lax.optimization_barrier(hidden_pos.astype(jnp.bfloat16)).astype(jnp.float32)
        rating_logits = visible_bias_rows + jnp.einsum("cm,rcjm->rcj", positive_lower_part, movie_weight_rows, precision=highest_rating)
        largest = jnp.max(rating_logits, axis=0, keepdims=True)
        exponent = jnp.exp(rating_logits - largest)
        softened = (exponent / jnp.sum(exponent, axis=0, keepdims=True)).astype(jnp.bfloat16)
        reconstructed_ratings = lax.optimization_barrier(softened).astype(jnp.float32) * usable[None]
        negative_statistics = jnp.einsum("drp,drpv->rv", reconstructed_ratings, movie_weight_rows, precision=highest_rating)
        hidden_neg = jax.nn.sigmoid(hid_bias[None, :] + negative_statistics)
        negative_low = lax.optimization_barrier(hidden_neg.astype(jnp.bfloat16)).astype(jnp.float32)
        contrib = observed_mask[..., None] * positive_lower_part[None, :, None, :] - reconstructed_ratings[..., None] * negative_low[None, :, None, :]
        weight_grad = weight_grad.at[:, movie_block].add(contrib)
        visible_grad = visible_grad.at[:, movie_block].add(observed_mask - reconstructed_ratings)
        hidden_grad = hidden_grad + jnp.sum(hidden_pos - hidden_neg, axis=0)
        return (weight_grad, visible_grad, hidden_grad), hidden_pos

    initial = (jnp.zeros((levels, movies, hidden), jnp.float32), jnp.zeros((levels, movies), jnp.float32), jnp.zeros((hidden,), jnp.float32))
    totals, hidden_rows = lax.scan(advance, initial, jnp.arange(block_count, dtype=jnp.int32))
    weight_grad, visible_grad, hidden_grad = totals
    return weight_grad, visible_grad, hidden_grad, hidden_rows.reshape(user_count, hidden)
```

```python
import functools

import jax
import jax.numpy as jnp
from jax import lax
from jax.experimental import pallas as pl
from jax.experimental.pallas import tpu as pltpu
from jax.sharding import PartitionSpec as P

LANES = 128
F32 = jnp.float32
BF16 = jnp.bfloat16
MIB = 1 << 20
TILES = (5, 4, 7, 10)
PARTS = (2, 4, 5, 7)
SENT = F32
TN = (((0,), (0,)), ((), ()))
NT = (((1,), (1,)), ((), ()))


def positive_kernel(codes_ref, source, partial_ref, rating_ref, table, shown, movie_s, grade_s, total, arrived):
    sources, local_users, slots = codes_ref.shape
    half = slots // 2
    local_movies = rating_ref.shape[0]
    columns = source.shape[0]
    levels = columns // local_movies
    tile = pick_tile(local_movies, TILES)
    chunks = row_chunks(columns, arrived.shape[0])
    copies = [
        pltpu.make_async_copy(source.at[pl.ds(at, size)], table.at[pl.ds(at, size)], arrived.at[i])
        for i, (at, size) in enumerate(chunks)
    ]
    for copy in copies:
        copy.start()

    rows = jnp.concatenate([codes_ref[i] for i in range(sources)], axis=0).astype(F32)
    turned = rows.T
    both = jnp.concatenate([turned[:half], turned[half:]], axis=1)
    movie = jnp.floor(both * 0.125)
    movie_s[...] = movie - (lax.axis_index("movie") * local_movies).astype(F32)
    grade_s[...] = both - movie * 8.0
    place = lax.broadcasted_iota(jnp.int32, (tile, LANES), 0).astype(F32).astype(BF16)

    for at in range(0, local_movies, tile):

        def add_slot(slot, found):
            movie = jnp.broadcast_to(movie_s[pl.ds(slot, 1), :] - float(at), (16, LANES)).astype(BF16)
            grade = jnp.broadcast_to(grade_s[pl.ds(slot, 1), :], (16, LANES)).astype(BF16)
            movie = jnp.tile(movie, (tile // 16, 1))
            grade = jnp.tile(grade, (tile // 16, 1))
            return jnp.where(place == movie, grade, found)

        found = lax.fori_loop(0, half, add_slot, jnp.full((tile, LANES), -1.0, BF16), unroll=16)
        wide = found.astype(F32)
        wide = jnp.maximum(wide, pltpu.roll(wide, LANES // 2, 1))
        rating_ref[at : at + tile, :] = wide.astype(BF16)
        for k in range(levels):
            first = k * local_movies + at
            shown[first : first + tile, :] = jnp.where(wide == float(k), 1.0, 0.0).astype(BF16)

    for i, (at, size) in enumerate(chunks):
        copies[i].wait()
        part = lax.dot_general(shown[at : at + size, :], table[at : at + size, :], TN, preferred_element_type=F32)
        total[...] = part if i == 0 else total[...] + part
    for i in range(sources):
        partial_ref[i] = total[i * local_users : (i + 1) * local_users, :].astype(partial_ref.dtype)


def negative_kernel(rows_ref, source, bias_ref, rating_ref, partial_ref, stats_ref, table, probs, total, arrived):
    sources, local_users, hidden = rows_ref.shape
    users = sources * local_users
    local_movies = rating_ref.shape[0]
    levels = source.shape[0] // local_movies
    tile = pick_tile(local_movies, TILES)
    tiles = range(local_movies // tile)
    block = levels * tile
    copies = [
        [
            pltpu.make_async_copy(
                source.at[pl.ds(k * local_movies + t * tile, tile)],
                table.at[pl.ds(t * block + k * tile, tile)],
                arrived.at[t, k],
            )
            for k in range(levels)
        ]
        for t in tiles
    ]
    for group in copies:
        for copy in group:
            copy.start()

    rows = jnp.concatenate([rows_ref[i].astype(F32) for i in range(sources)], axis=0)
    probs[...] = jnp.concatenate([rows, rows], axis=0).T.astype(BF16)
    first = lax.broadcasted_iota(jnp.int32, (tile, LANES), 1) < LANES // 2

    def logits(t):
        for copy in copies[t]:
            copy.wait()
        return jnp.dot(table[t * block : (t + 1) * block, :], probs[...], preferred_element_type=F32)

    ready = logits(0)
    for t in tiles:
        following = logits(t + 1) if t + 1 < len(tiles) else None
        own = slice(t * tile, (t + 1) * tile)
        bias = bias_ref[own, :]
        level = [ready[k * tile : (k + 1) * tile] + bias[:, k : k + 1] for k in range(levels)]
        largest = functools.reduce(jnp.maximum, level)
        level = [jnp.exp(x - largest) for x in level]
        scale = 1.0 / functools.reduce(jnp.add, level)
        rating = rating_ref[own, :].astype(F32)
        scale = jnp.where(rating >= 0.0, scale, 0.0)
        stats = []
        for k in range(levels):
            shown = jnp.where(rating == float(k), 1.0, 0.0)
            stats.append(jnp.where(first, shown, -(level[k] * scale)).astype(BF16))
            at = k * local_movies + t * tile
            stats_ref[at : at + tile, :] = stats[k]
        stats = jnp.concatenate(stats, axis=0)
        part = lax.dot_general(
            stats, table[t * block : (t + 1) * block, :], TN, preferred_element_type=F32
        )
        total[...] = part if t == 0 else total[...] + part
        ready = following
    for i in range(sources):
        row = users + i * local_users
        partial_ref[i] = (-total[row : row + local_users, :]).astype(partial_ref.dtype)


def positive_rows_kernel(parts_ref, bias_ref, own_ref, sent_ref):
    sources = parts_ref.shape[0]
    summed = functools.reduce(jnp.add, [parts_ref[i].astype(F32) for i in range(sources)])
    own = jax.nn.sigmoid(bias_ref[...] + summed)
    own_ref[...] = own
    low = own.astype(BF16)
    for i in range(sources):
        sent_ref[i] = low


def negative_rows_kernel(parts_ref, bias_ref, positive_ref, _, sent_ref):
    sources, local_users, hidden = parts_ref.shape
    side = 2 * hidden // local_users
    summed = functools.reduce(jnp.add, [parts_ref[i].astype(F32) for i in range(sources)])
    own = jax.nn.sigmoid(bias_ref[...] + summed)
    difference = jnp.sum(positive_ref[...] - own, axis=0, keepdims=True)
    high = difference.astype(BF16).astype(F32)
    rest = difference - high
    pieces = hidden // side
    split = [x[:, i * side : (i + 1) * side] for x in (high, rest) for i in range(pieces)]
    low = jnp.concatenate([own, jnp.concatenate(split, axis=0)], axis=1).astype(BF16)
    for i in range(sources):
        sent_ref[i] = low


def gradient_kernel(stats_a, stats_b, pos_a, pos_b, neg_a, neg_b, target, visible_ref, hidden_ref, lhs, rhs, slots, sent):
    sources, local_users, hidden = pos_a.shape
    levels, local_movies, _ = stats_a.shape
    side = neg_a.shape[2] - hidden
    pieces = hidden // side
    buffers, rows, _ = slots.shape
    parts = local_movies // rows
    mine = pl.multiple_of(lax.axis_index("user") * LANES, LANES)
    other = pl.multiple_of(LANES - mine, LANES)

    sides = []
    for at, pos, neg in ((mine, pos_a, neg_a), (other, pos_b, neg_b)):
        wide = [neg[i].astype(F32) for i in range(sources)]
        block = [pos[i].astype(F32) for i in range(sources)] + [x[:, :hidden] for x in wide]
        rhs[pl.ds(at, LANES), :] = jnp.concatenate(block, axis=0).astype(BF16)
        sides.append(functools.reduce(jnp.add, [x[:, hidden:] for x in wide]))
    both = sides[0] + sides[1]
    both = both[:pieces] + both[pieces:]
    for i in range(pieces):
        hidden_ref[:, i * side : (i + 1) * side] = both[i : i + 1]
    ones = jnp.ones((8, LANES), BF16)

    def send(level, part, slot):
        place = target.at[level, pl.ds(part * rows, rows)]
        return pltpu.make_async_copy(slots.at[slot], place, sent.at[slot])

    def one_level(level, carry):
        a, b = stats_a[level], stats_b[level]
        lhs[:, pl.ds(mine, LANES)] = a
        lhs[:, pl.ds(other, LANES)] = b
        for part in range(parts):
            count = level * parts + part
            slot = lax.rem(count, buffers)

            @pl.when(count >= buffers)
            def _():
                send(level, part, slot).wait()

            block = lhs[part * rows : (part + 1) * rows, :]
            slots[slot] = jnp.dot(block, rhs[...], preferred_element_type=F32)
            send(level, part, slot).start()
        summed = lax.dot_general(ones, a, NT, preferred_element_type=F32) + lax.dot_general(
            ones, b, NT, preferred_element_type=F32
        )
        visible_ref[pl.ds(level, 1), :] = summed[:1]
        return carry

    lax.fori_loop(0, levels, one_level, 0)
    for slot in range(min(buffers, levels * parts)):
        send(0, 0, slot).wait()


def whole(shape):
    return pl.BlockSpec(shape, lambda *_: (0,) * len(shape))


def params(limit):
    return pltpu.CompilerParams(vmem_limit_bytes=limit)


def exchange(x):
    return lax.all_to_all(x, "movie", split_axis=0, concat_axis=0, tiled=True)


def pick_tile(local_movies, parts):
    for count in parts:
        if local_movies % count == 0 and (local_movies // count) % 16 == 0:
            return local_movies // count
    return None


def row_chunks(rows, count):
    blocks = pl.cdiv(rows, 256)
    edges = [min(rows, 256 * (blocks * i // count)) for i in range(count)] + [rows]
    return [(a, b - a) for a, b in zip(edges, edges[1:])]


def on_device_kernels(movie_ids, ratings, valid, weights, vis_bias, hid_bias):
    owners = lax.axis_size("movie")
    local_users, slots = movie_ids.shape
    levels, local_movies, hidden = weights.shape
    columns = levels * local_movies
    users = owners * local_users
    tile = pick_tile(local_movies, TILES)
    rows = pick_tile(local_movies, PARTS)
    swap = [(0, 1), (1, 0)]
    matmul = 2 * users * columns * hidden
    table_bytes = weights.size * 2

    code = jnp.where(valid == 1, movie_ids * 8 + ratings, -8)
    codes = exchange(jnp.broadcast_to(code[None], (owners, local_users, slots)))
    table = pltpu.with_memory_space_constraint(weights.reshape(columns, hidden), pltpu.HBM)
    vis_rows = vis_bias.T
    bias_row = hid_bias[None, :]
    table_scratch = pltpu.VMEM((columns, hidden), BF16)
    total_scratch = pltpu.VMEM((LANES, hidden), F32)
    vmem = pl.BlockSpec(memory_space=pltpu.VMEM)
    table_spec = pl.BlockSpec(memory_space=pltpu.HBM)
    parts_shape = (owners, local_users, hidden)

    positive_part, rating = pl.pallas_call(
        positive_kernel,
        in_specs=[vmem, table_spec],
        out_specs=[vmem, vmem],
        out_shape=[
            jax.ShapeDtypeStruct(parts_shape, SENT),
            jax.ShapeDtypeStruct((local_movies, LANES), BF16),
        ],
        scratch_shapes=[
            table_scratch,
            pltpu.VMEM((columns, LANES), BF16),
            pltpu.VMEM((slots // 2, LANES), F32),
            pltpu.VMEM((slots // 2, LANES), F32),
            total_scratch,
            pltpu.SemaphoreType.DMA((4,)),
        ],
        compiler_params=params(32 * MIB),
        cost_estimate=pl.CostEstimate(flops=matmul, bytes_accessed=table_bytes, transcendentals=0),
        name="positive",
    )(codes, table)

    positive_own, sent = pl.pallas_call(
        positive_rows_kernel,
        out_shape=[
            jax.ShapeDtypeStruct((local_users, hidden), F32),
            jax.ShapeDtypeStruct(parts_shape, BF16),
        ],
        compiler_params=params(8 * MIB),
        name="positive_rows",
    )(exchange(positive_part), bias_row)
    pos_a = exchange(sent)
    pos_b = lax.ppermute(pos_a, "user", swap)

    negative_part, stats_a = pl.pallas_call(
        negative_kernel,
        in_specs=[vmem, table_spec, vmem, vmem],
        out_specs=[vmem, vmem],
        out_shape=[
            jax.ShapeDtypeStruct(parts_shape, SENT),
            jax.ShapeDtypeStruct((columns, LANES), BF16),
        ],
        scratch_shapes=[
            table_scratch,
            pltpu.VMEM((hidden, LANES), BF16),
            total_scratch,
            pltpu.SemaphoreType.DMA((local_movies // tile, levels)),
        ],
        compiler_params=params(32 * MIB),
        cost_estimate=pl.CostEstimate(flops=2 * matmul, bytes_accessed=table_bytes, transcendentals=0),
        name="negative",
    )(pos_a, table, vis_rows, rating)
    stats_a = stats_a.reshape(levels, local_movies, LANES)
    stats_b = lax.ppermute(stats_a, "user", swap)

    sent = pl.pallas_call(
        negative_rows_kernel,
        in_specs=[vmem, vmem, vmem, pl.BlockSpec(memory_space=pl.ANY)],
        out_shape=jax.ShapeDtypeStruct((owners, local_users, hidden + 2 * hidden // local_users), BF16),
        compiler_params=params(8 * MIB),
        name="negative_rows",
    )(exchange(negative_part), bias_row, positive_own, pos_b)
    neg_a = exchange(sent)
    neg_b = lax.ppermute(neg_a, "user", swap)

    weight_grad, visible_grad, hidden_grad = pl.pallas_call(
        gradient_kernel,
        in_specs=[vmem] * 6,
        out_specs=[pl.BlockSpec(memory_space=pltpu.HBM), vmem, vmem],
        out_shape=[
            jax.ShapeDtypeStruct(weights.shape, F32),
            jax.ShapeDtypeStruct((levels, local_movies), F32),
            jax.ShapeDtypeStruct((1, hidden), F32),
        ],
        scratch_shapes=[
            pltpu.VMEM((local_movies, 2 * LANES), BF16),
            pltpu.VMEM((2 * LANES, hidden), BF16),
            pltpu.VMEM((3, rows, hidden), F32),
            pltpu.SemaphoreType.DMA((3,)),
        ],
        compiler_params=params(32 * MIB),
        cost_estimate=pl.CostEstimate(flops=4 * matmul, bytes_accessed=2 * table_bytes, transcendentals=0),
        name="gradient",
    )(stats_a, stats_b, pos_a, pos_b, neg_a, neg_b)
    return weight_grad, visible_grad, hidden_grad[0], positive_own


def fits_kernels(mesh, local_users, slots, levels, local_movies, hidden):
    users = mesh.shape["movie"] * local_users
    return (
        mesh.shape["user"] == 2
        and users == LANES // 2
        and slots % 16 == 0
        and hidden % (LANES * local_users) == 0
        and local_users == 4
        and levels < 8
        and pick_tile(local_movies, TILES) is not None
        and pick_tile(local_movies, PARTS) is not None
    )


def reconstruct(hidden_rows, weight_table, bias_row, rated_mask, levels):
    group_rows = hidden_rows.shape[0]
    rating_logits = (
        lax.dot_general(
            hidden_rows, weight_table, (((1,), (1,)), ((), ())), preferred_element_type=jnp.float32
        )
        + bias_row[None, :]
    )
    shaped = rating_logits.reshape(group_rows, levels, -1)
    largest = jnp.max(shaped, axis=1, keepdims=True)
    exponent = jnp.exp(shaped - largest)
    softened = (exponent / jnp.sum(exponent, axis=1, keepdims=True)).astype(jnp.bfloat16)
    return (softened * rated_mask[:, None, :]).reshape(group_rows, -1)


def hidden_phase(visible, weight_table, hid_bias, local_users, device_index):
    combined = jnp.dot(visible, weight_table, preferred_element_type=jnp.float32)
    all_probs = jax.nn.sigmoid(hid_bias[None, :] + lax.psum(combined, "movie"))
    own_rows = lax.dynamic_slice_in_dim(all_probs, device_index * local_users, local_users, 0)
    return (own_rows, all_probs.astype(jnp.bfloat16))


def on_device(movie_ids, ratings, valid, weights, vis_bias, hid_bias):
    owners = lax.axis_size("movie")
    device_index = lax.axis_index("movie")
    local_users, slot_count = movie_ids.shape
    levels, local_movies, hidden = weights.shape
    columns = levels * local_movies
    group_rows = owners * local_users
    capacity = max(2, 3 * local_users * slot_count // owners)
    flat_ids = movie_ids.reshape(-1)
    owner_ids = flat_ids // local_movies
    column_ids = ratings.reshape(-1) * local_movies + flat_ids % local_movies
    user_ids = jnp.arange(local_users * slot_count, dtype=jnp.int32) // slot_count
    usable = valid.reshape(-1) == 1
    matches = (owner_ids[:, None] == jnp.arange(owners, dtype=jnp.int32)[None, :]) & usable[:, None]
    ranking = jnp.cumsum(matches.astype(jnp.int32), axis=0) - 1
    placed = jnp.sum(jnp.where(matches, ranking, 0), axis=1)
    target = jnp.where(usable, owner_ids, owners)
    user_slots = (
        jnp.zeros((owners, capacity), jnp.int32).at[target, placed].set(user_ids, mode="drop")
    )
    column_slots = (
        jnp.full((owners, capacity), -1, jnp.int32).at[target, placed].set(column_ids, mode="drop")
    )
    got_users, got_columns = (
        lax.all_to_all(user_slots, "movie", split_axis=0, concat_axis=0, tiled=True),
        lax.all_to_all(column_slots, "movie", split_axis=0, concat_axis=0, tiled=True),
    )
    user_hot = (got_users[:, :, None] == jnp.arange(local_users, dtype=jnp.int32)).astype(
        jnp.bfloat16
    )
    column_hot = (got_columns[:, :, None] == jnp.arange(columns, dtype=jnp.int32)).astype(
        jnp.bfloat16
    )
    shown = jnp.einsum("ncu,ncj->nuj", user_hot, column_hot, preferred_element_type=jnp.float32)
    shown = shown.reshape(group_rows, columns).astype(jnp.bfloat16)
    rated_mask = jnp.sum(shown.reshape(group_rows, levels, local_movies), axis=1)
    weight_table = weights.reshape(columns, hidden)
    positive_own, positive_group = hidden_phase(
        shown, weight_table, hid_bias, local_users, device_index
    )
    reconstructed_ratings = reconstruct(
        positive_group, weight_table, vis_bias.reshape(columns), rated_mask, levels
    )
    negative_own, negative_group = hidden_phase(
        reconstructed_ratings, weight_table, hid_bias, local_users, device_index
    )
    contract = (((0,), (0,)), ((), ()))
    weight_grad = lax.dot_general(
        shown, positive_group, contract, preferred_element_type=jnp.float32
    )
    weight_grad = weight_grad - lax.dot_general(
        reconstructed_ratings, negative_group, contract, preferred_element_type=jnp.float32
    )
    visible_grad = jnp.sum(shown.astype(jnp.float32), axis=0) - jnp.sum(
        reconstructed_ratings.astype(jnp.float32), axis=0
    )
    weight_grad, visible_grad = lax.psum((weight_grad, visible_grad), "user")
    hidden_grad = lax.psum(jnp.sum(positive_own - negative_own, axis=0), ("movie", "user"))
    return (
        weight_grad.reshape(levels, local_movies, hidden),
        visible_grad.reshape(levels, local_movies),
        hidden_grad,
        positive_own,
    )


def solution(mesh):
    in_specs = (
        P(("movie", "user"), None),
        P(("movie", "user"), None),
        P(("movie", "user"), None),
        P(None, "movie", None),
        P(None, "movie"),
        P(),
    )
    out_specs = (P(None, "movie", None), P(None, "movie"), P(), P(("movie", "user"), None))

    def step(movie_ids, ratings, valid, weights, vis_bias, hid_bias):
        owners = mesh.shape["movie"]
        local_users = movie_ids.shape[0] // (owners * mesh.shape["user"])
        levels, movies, hidden = weights.shape
        fits = fits_kernels(mesh, local_users, movie_ids.shape[1], levels, movies // owners, hidden)
        return jax.shard_map(
            on_device_kernels if fits else on_device,
            mesh=mesh,
            in_specs=in_specs,
            out_specs=out_specs,
            check_vma=False,
        )(movie_ids, ratings, valid, weights, vis_bias, hid_bias)

    return step
```

```python
import functools

import jax
import jax.numpy as jnp
from jax import lax
from jax.experimental import pallas as pl
from jax.experimental.pallas import tpu as pltpu
from jax.sharding import PartitionSpec as P

LANES = 128
F32 = jnp.float32
BF16 = jnp.bfloat16
MIB = 1 << 20
TILES = (7, 5, 4, 10)
PARTS = (2, 4, 5, 7)
WIDE_TILE = 256
TN = (((0,), (0,)), ((), ()))
NT = (((1,), (1,)), ((), ()))


def positive_kernel(codes_ref, source, partial_ref, rating_ref, head, table, shown, movie_s, grade_s, total, arrived):
    sources, local_users, slots = codes_ref.shape
    half = slots // 2
    local_movies = rating_ref.shape[0]
    levels = source.shape[0] // local_movies
    tile = head.shape[0] // levels
    rest = local_movies - tile
    blocks = [(0, levels * tile, head, 0)]
    blocks += [(levels * tile + k * rest, rest, table, k * rest) for k in range(levels)]
    copies = []
    for k in range(levels):
        first = k * local_movies
        copies.append((source.at[pl.ds(first, tile)], head.at[pl.ds(k * tile, tile)]))
    for k in range(levels):
        first = k * local_movies + tile
        copies.append((source.at[pl.ds(first, rest)], table.at[pl.ds(k * rest, rest)]))
    copies = [pltpu.make_async_copy(*pair, arrived.at[i]) for i, pair in enumerate(copies)]
    for copy in copies:
        copy.start()

    rows = jnp.concatenate([codes_ref[i] for i in range(sources)], axis=0).astype(F32)
    turned = rows.T
    both = jnp.concatenate([turned[:half], turned[half:]], axis=1)
    movie = jnp.floor(both * 0.125)
    movie_s[...] = movie - (lax.axis_index("movie") * local_movies).astype(F32)
    grade_s[...] = both - movie * 8.0
    place = lax.broadcasted_iota(jnp.int32, (tile, LANES), 0).astype(F32).astype(BF16)

    for at in range(0, local_movies, tile):

        def add_slot(slot, found):
            movie = jnp.broadcast_to(movie_s[pl.ds(slot, 1), :] - float(at), (16, LANES)).astype(BF16)
            grade = jnp.broadcast_to(grade_s[pl.ds(slot, 1), :], (16, LANES)).astype(BF16)
            movie = jnp.tile(movie, (tile // 16, 1))
            grade = jnp.tile(grade, (tile // 16, 1))
            return jnp.where(place == movie, grade, found)

        found = lax.fori_loop(0, half, add_slot, jnp.full((tile, LANES), -1.0, BF16), unroll=16)
        wide = found.astype(F32)
        wide = jnp.maximum(wide, pltpu.roll(wide, LANES // 2, 1))
        rating_ref[at : at + tile, :] = wide.astype(BF16)
        for k in range(levels):
            first = k * tile if at == 0 else levels * tile + k * rest + at - tile
            shown[first : first + tile, :] = jnp.where(wide == float(k), 1.0, 0.0).astype(BF16)

    waits = [copies[:levels]] + [[copy] for copy in copies[levels:]]
    for i, (at, size, ref, start) in enumerate(blocks):
        for copy in waits[i]:
            copy.wait()
        part = lax.dot_general(
            shown[at : at + size, :], ref[start : start + size, :], TN, preferred_element_type=F32
        )
        total[...] = part if i == 0 else total[...] + part
    for i in range(sources):
        partial_ref[i] = total[i * local_users : (i + 1) * local_users, :].astype(partial_ref.dtype)


def negative_kernel(rows_ref, source, head, bias_ref, rating_ref, own_ref, partial_ref, stats_ref, own_out, table, probs, bias_s, total, arrived, sent):
    sources, local_users, hidden = rows_ref.shape
    users = sources * local_users
    local_movies = rating_ref.shape[0]
    levels = source.shape[0] // local_movies
    held = head.shape[0] // levels
    tiles = movie_tiles(held, local_movies)
    copies = [[]] + [
        [
            pltpu.make_async_copy(
                source.at[pl.ds(k * local_movies + at, tile)],
                table.at[pl.ds(levels * (at - held) + k * tile, tile)],
                arrived.at[t, k],
            )
            for k in range(levels)
        ]
        for t, (at, tile) in enumerate(tiles[1:])
    ]
    for group in copies:
        for copy in group:
            copy.start()

    own_copy = pltpu.make_async_copy(own_ref, own_out, sent)
    own_copy.start()
    spare = jnp.zeros((8 - levels, local_movies), F32)
    bias_s[...] = jnp.concatenate([bias_ref[...], spare], axis=0).T
    rows = jnp.concatenate([rows_ref[i].astype(F32) for i in range(sources)], axis=0)
    probs[...] = jnp.concatenate([rows, rows], axis=0).T.astype(BF16)
    def block(t):
        at, tile = tiles[t]
        return head[...] if t == 0 else table[levels * (at - held) : levels * (at - held + tile), :]

    def logits(t):
        for copy in copies[t]:
            copy.wait()
        return jnp.dot(block(t), probs[...], preferred_element_type=F32)

    ready = logits(0)
    for t, (start, tile) in enumerate(tiles):
        following = logits(t + 1) if t + 1 < len(tiles) else None
        first = lax.broadcasted_iota(jnp.int32, (tile, LANES), 1) < LANES // 2
        own = slice(start, start + tile)
        bias = bias_s[own, :]
        level = [ready[k * tile : (k + 1) * tile] + bias[:, k : k + 1] for k in range(levels)]
        largest = functools.reduce(jnp.maximum, level)
        level = [jnp.exp(x - largest) for x in level]
        scale = 1.0 / functools.reduce(jnp.add, level)
        rating = rating_ref[own, :].astype(F32)
        scale = jnp.where(rating >= 0.0, scale, 0.0)
        stats = []
        for k in range(levels):
            shown = jnp.where(rating == float(k), 1.0, 0.0)
            stats.append(jnp.where(first, shown, -(level[k] * scale)).astype(BF16))
            at = k * local_movies + start
            stats_ref[at : at + tile, :] = stats[k]
        stats = jnp.concatenate(stats, axis=0)
        part = lax.dot_general(
            stats, block(t), TN, preferred_element_type=F32
        )
        total[...] = part if t == 0 else total[...] + part
        ready = following
    for i in range(sources):
        row = users + i * local_users
        partial_ref[i] = (-total[row : row + local_users, :]).astype(partial_ref.dtype)
    own_copy.wait()


def positive_rows_kernel(parts_ref, bias_ref, own_ref, sent_ref):
    sources = parts_ref.shape[0]
    summed = functools.reduce(jnp.add, [parts_ref[i].astype(F32) for i in range(sources)])
    own = jax.nn.sigmoid(bias_ref[...] + summed)
    own_ref[...] = own
    low = own.astype(BF16)
    for i in range(sources):
        sent_ref[i] = low


def negative_rows_kernel(parts_ref, bias_ref, positive_ref, sent_ref):
    sources, local_users, hidden = parts_ref.shape
    side = 2 * hidden // local_users
    summed = functools.reduce(jnp.add, [parts_ref[i].astype(F32) for i in range(sources)])
    own = jax.nn.sigmoid(bias_ref[...] + summed)
    difference = jnp.sum(positive_ref[...] - own, axis=0, keepdims=True)
    high = difference.astype(BF16).astype(F32)
    rest = difference - high
    pieces = hidden // side
    split = [x[:, i * side : (i + 1) * side] for x in (high, rest) for i in range(pieces)]
    low = jnp.concatenate([own, jnp.concatenate(split, axis=0)], axis=1).astype(BF16)
    for i in range(sources):
        sent_ref[i] = low


def gathered_rows_kernel(pos_ref, neg_ref, rows_ref):
    sources, _, hidden = pos_ref.shape
    wide = [neg_ref[i].astype(F32) for i in range(sources)]
    block = [pos_ref[i].astype(F32) for i in range(sources)] + [x[:, :hidden] for x in wide]
    sides = functools.reduce(jnp.add, [x[:, hidden:] for x in wide])
    pieces = sides.shape[0] // 2
    sides = sides[:pieces] + sides[pieces:]
    rest = jnp.concatenate([sides[i : i + 1] for i in range(pieces)], axis=1)
    terms = []
    for _ in range(3):
        terms.append(rest.astype(BF16).astype(F32))
        rest = rest - terms[-1]
    spare = jnp.zeros((rows_ref.shape[0] - LANES - len(terms), hidden), F32)
    rows_ref[...] = jnp.concatenate(block + terms + [spare], axis=0).astype(BF16)


def gradient_kernel(stats_a, stats_b, rows_a, rows_b, target, visible_out, hidden_out, stats_s, visible_ref, hidden_ref, lhs, rhs, slots, sent, got, done):
    levels, local_movies, _ = stats_a.shape
    buffers, rows, _ = slots.shape
    parts = local_movies // rows
    mine = pl.multiple_of(lax.axis_index("user") * LANES, LANES)
    other = pl.multiple_of(LANES - mine, LANES)

    fetch = [pltpu.make_async_copy(stats_b.at[i], stats_s.at[i], got.at[i]) for i in range(levels)]
    for copy in fetch:
        copy.start()
    rhs[pl.ds(mine, LANES), :] = rows_a[:LANES, :]
    rhs[pl.ds(other, LANES), :] = rows_b[:LANES, :]
    sums = [jnp.sum(ref[LANES:, :].astype(F32), axis=0, keepdims=True) for ref in (rows_a, rows_b)]
    hidden_ref[...] = sums[0] + sums[1]
    ones = jnp.ones((8, LANES), BF16)

    def send(level, part, slot):
        place = target.at[level, pl.ds(part * rows, rows)]
        return pltpu.make_async_copy(slots.at[slot], place, sent.at[slot])

    def one_level(level, carry):
        pltpu.make_async_copy(stats_b.at[level], stats_s.at[level], got.at[level]).wait()
        a, b = stats_a[level], stats_s[level]
        lhs[:, pl.ds(mine, LANES)] = a
        lhs[:, pl.ds(other, LANES)] = b
        for part in range(parts):
            count = level * parts + part
            slot = lax.rem(count, buffers)

            @pl.when(count >= buffers)
            def _():
                send(level, part, slot).wait()

            block = lhs[part * rows : (part + 1) * rows, :]
            slots[slot] = jnp.dot(block, rhs[...], preferred_element_type=F32)
            send(level, part, slot).start()
        summed = lax.dot_general(ones, a, NT, preferred_element_type=F32) + lax.dot_general(
            ones, b, NT, preferred_element_type=F32
        )
        visible_ref[pl.ds(level, 1), :] = summed[:1]
        return carry

    lax.fori_loop(0, levels, one_level, 0)
    small = [
        pltpu.make_async_copy(visible_ref, visible_out, done.at[0]),
        pltpu.make_async_copy(hidden_ref, hidden_out, done.at[1]),
    ]
    for copy in small:
        copy.start()
    for slot in range(min(buffers, levels * parts)):
        send(0, 0, slot).wait()
    for copy in small:
        copy.wait()


def whole(shape):
    return pl.BlockSpec(shape, lambda *_: (0,) * len(shape))


def params(limit):
    return pltpu.CompilerParams(vmem_limit_bytes=limit)


def exchange(x):
    return lax.all_to_all(x, "movie", split_axis=0, concat_axis=0, tiled=True)


def pick_tile(local_movies, parts):
    for count in parts:
        if local_movies % count == 0 and (local_movies // count) % 16 == 0:
            return local_movies // count
    return None


def movie_tiles(held, movies):
    wide, left = divmod(movies - held, WIDE_TILE)
    sizes = [held] + [WIDE_TILE] * wide
    sizes += [left // 2] * 2 if left and left % 32 == 0 else [left] * (left > 0)
    return [(sum(sizes[:i]), size) for i, size in enumerate(sizes)]


def on_device_kernels(movie_ids, ratings, valid, weights, vis_bias, hid_bias):
    owners = lax.axis_size("movie")
    local_users, slots = movie_ids.shape
    levels, local_movies, hidden = weights.shape
    columns = levels * local_movies
    users = owners * local_users
    tile = pick_tile(local_movies, TILES)
    part = pick_tile(local_movies, PARTS)
    swap = [(0, 1), (1, 0)]
    matmul = 2 * users * columns * hidden
    table_bytes = weights.size * 2

    code = jnp.where(valid == 1, movie_ids * 8 + ratings, -8)
    codes = exchange(jnp.broadcast_to(code[None], (owners, local_users, slots)))
    table = pltpu.with_memory_space_constraint(weights.reshape(columns, hidden), pltpu.HBM)
    bias_row = hid_bias[None, :]
    table_scratch = pltpu.VMEM((levels * (local_movies - tile), hidden), BF16)
    total_scratch = pltpu.VMEM((LANES, hidden), F32)
    vmem = pl.BlockSpec(memory_space=pltpu.VMEM)
    table_spec = pl.BlockSpec(memory_space=pltpu.HBM)
    parts_shape = (owners, local_users, hidden)

    positive_part, rating, head = pl.pallas_call(
        positive_kernel,
        in_specs=[vmem, table_spec],
        out_specs=[vmem, vmem, vmem],
        out_shape=[
            pltpu.VMEM(parts_shape, F32),
            jax.ShapeDtypeStruct((local_movies, LANES), BF16),
            pltpu.VMEM((levels * tile, hidden), BF16),
        ],
        scratch_shapes=[
            table_scratch,
            pltpu.VMEM((columns, LANES), BF16),
            pltpu.VMEM((slots // 2, LANES), F32),
            pltpu.VMEM((slots // 2, LANES), F32),
            total_scratch,
            pltpu.SemaphoreType.DMA((2 * levels,)),
        ],
        compiler_params=params(32 * MIB),
        cost_estimate=pl.CostEstimate(flops=matmul, bytes_accessed=table_bytes, transcendentals=0),
        name="positive",
    )(codes, table)

    positive_own, sent = pl.pallas_call(
        positive_rows_kernel,
        out_shape=[
            pltpu.VMEM((local_users, hidden), F32),
            pltpu.VMEM(parts_shape, BF16),
        ],
        compiler_params=params(8 * MIB),
        name="positive_rows",
    )(exchange(positive_part), bias_row)
    pos_a = exchange(sent)

    negative_part, stats_a, positive_out = pl.pallas_call(
        negative_kernel,
        in_specs=[vmem, table_spec, vmem, vmem, vmem, vmem],
        out_specs=[vmem, vmem, pl.BlockSpec(memory_space=pltpu.HBM)],
        out_shape=[
            pltpu.VMEM(parts_shape, BF16),
            jax.ShapeDtypeStruct((columns, LANES), BF16),
            jax.ShapeDtypeStruct(positive_own.shape, F32),
        ],
        scratch_shapes=[
            table_scratch,
            pltpu.VMEM((hidden, LANES), BF16),
            pltpu.VMEM((local_movies, 8), F32),
            total_scratch,
            pltpu.SemaphoreType.DMA((len(movie_tiles(tile, local_movies)), levels)),
            pltpu.SemaphoreType.DMA,
        ],
        compiler_params=params(32 * MIB),
        cost_estimate=pl.CostEstimate(flops=2 * matmul, bytes_accessed=table_bytes, transcendentals=0),
        name="negative",
    )(pos_a, table, head, vis_bias, rating, positive_own)
    stats_a = stats_a.reshape(levels, local_movies, LANES)
    stats_b = lax.ppermute(stats_a, "user", swap)

    sent = pl.pallas_call(
        negative_rows_kernel,
        out_shape=pltpu.VMEM((owners, local_users, hidden + 2 * hidden // local_users), BF16),
        compiler_params=params(8 * MIB),
        name="negative_rows",
    )(exchange(negative_part), bias_row, positive_own)
    rows_a = pl.pallas_call(
        gathered_rows_kernel,
        out_shape=pltpu.VMEM((LANES + 16, hidden), BF16),
        compiler_params=params(8 * MIB),
        name="gathered_rows",
    )(pos_a, exchange(sent))
    rows_b = lax.ppermute(rows_a, "user", swap)
    weight_grad, visible_grad, hidden_grad = pl.pallas_call(
        gradient_kernel,
        in_specs=[vmem, pl.BlockSpec(memory_space=pl.ANY)] + [vmem] * 2,
        out_specs=[pl.BlockSpec(memory_space=pltpu.HBM)] * 3,
        out_shape=[
            jax.ShapeDtypeStruct(weights.shape, F32),
            jax.ShapeDtypeStruct((levels, local_movies), F32),
            jax.ShapeDtypeStruct((1, hidden), F32),
        ],
        scratch_shapes=[
            pltpu.VMEM(stats_a.shape, BF16),
            pltpu.VMEM((levels, local_movies), F32),
            pltpu.VMEM((1, hidden), F32),
            pltpu.VMEM((local_movies, 2 * LANES), BF16),
            pltpu.VMEM((2 * LANES, hidden), BF16),
            pltpu.VMEM((3, part, hidden), F32),
            pltpu.SemaphoreType.DMA((3,)),
            pltpu.SemaphoreType.DMA((levels,)),
            pltpu.SemaphoreType.DMA((2,)),
        ],
        compiler_params=params(32 * MIB),
        cost_estimate=pl.CostEstimate(flops=4 * matmul, bytes_accessed=2 * table_bytes, transcendentals=0),
        name="gradient",
    )(stats_a, stats_b, rows_a, rows_b)
    return weight_grad, visible_grad, hidden_grad[0], positive_out


def fits_kernels(mesh, local_users, slots, levels, local_movies, hidden):
    users = mesh.shape["movie"] * local_users
    return (
        mesh.shape["user"] == 2
        and users == LANES // 2
        and slots % 16 == 0
        and hidden % (LANES * local_users) == 0
        and local_users == 4
        and levels < 8
        and pick_tile(local_movies, TILES) is not None
        and pick_tile(local_movies, PARTS) is not None
    )


def reconstruct(hidden_rows, weight_table, bias_row, rated_mask, levels):
    group_rows = hidden_rows.shape[0]
    rating_logits = (
        lax.dot_general(
            hidden_rows, weight_table, (((1,), (1,)), ((), ())), preferred_element_type=jnp.float32
        )
        + bias_row[None, :]
    )
    shaped = rating_logits.reshape(group_rows, levels, -1)
    largest = jnp.max(shaped, axis=1, keepdims=True)
    exponent = jnp.exp(shaped - largest)
    softened = (exponent / jnp.sum(exponent, axis=1, keepdims=True)).astype(jnp.bfloat16)
    return (softened * rated_mask[:, None, :]).reshape(group_rows, -1)


def hidden_phase(visible, weight_table, hid_bias, local_users, device_index):
    combined = jnp.dot(visible, weight_table, preferred_element_type=jnp.float32)
    all_probs = jax.nn.sigmoid(hid_bias[None, :] + lax.psum(combined, "movie"))
    own_rows = lax.dynamic_slice_in_dim(all_probs, device_index * local_users, local_users, 0)
    return (own_rows, all_probs.astype(jnp.bfloat16))


def on_device(movie_ids, ratings, valid, weights, vis_bias, hid_bias):
    owners = lax.axis_size("movie")
    device_index = lax.axis_index("movie")
    local_users, slot_count = movie_ids.shape
    levels, local_movies, hidden = weights.shape
    columns = levels * local_movies
    group_rows = owners * local_users
    capacity = max(2, 3 * local_users * slot_count // owners)
    flat_ids = movie_ids.reshape(-1)
    owner_ids = flat_ids // local_movies
    column_ids = ratings.reshape(-1) * local_movies + flat_ids % local_movies
    user_ids = jnp.arange(local_users * slot_count, dtype=jnp.int32) // slot_count
    usable = valid.reshape(-1) == 1
    matches = (owner_ids[:, None] == jnp.arange(owners, dtype=jnp.int32)[None, :]) & usable[:, None]
    ranking = jnp.cumsum(matches.astype(jnp.int32), axis=0) - 1
    placed = jnp.sum(jnp.where(matches, ranking, 0), axis=1)
    target = jnp.where(usable, owner_ids, owners)
    user_slots = (
        jnp.zeros((owners, capacity), jnp.int32).at[target, placed].set(user_ids, mode="drop")
    )
    column_slots = (
        jnp.full((owners, capacity), -1, jnp.int32).at[target, placed].set(column_ids, mode="drop")
    )
    got_users, got_columns = (
        lax.all_to_all(user_slots, "movie", split_axis=0, concat_axis=0, tiled=True),
        lax.all_to_all(column_slots, "movie", split_axis=0, concat_axis=0, tiled=True),
    )
    user_hot = (got_users[:, :, None] == jnp.arange(local_users, dtype=jnp.int32)).astype(
        jnp.bfloat16
    )
    column_hot = (got_columns[:, :, None] == jnp.arange(columns, dtype=jnp.int32)).astype(
        jnp.bfloat16
    )
    shown = jnp.einsum("ncu,ncj->nuj", user_hot, column_hot, preferred_element_type=jnp.float32)
    shown = shown.reshape(group_rows, columns).astype(jnp.bfloat16)
    rated_mask = jnp.sum(shown.reshape(group_rows, levels, local_movies), axis=1)
    weight_table = weights.reshape(columns, hidden)
    positive_own, positive_group = hidden_phase(
        shown, weight_table, hid_bias, local_users, device_index
    )
    reconstructed_ratings = reconstruct(
        positive_group, weight_table, vis_bias.reshape(columns), rated_mask, levels
    )
    negative_own, negative_group = hidden_phase(
        reconstructed_ratings, weight_table, hid_bias, local_users, device_index
    )
    contract = (((0,), (0,)), ((), ()))
    weight_grad = lax.dot_general(
        shown, positive_group, contract, preferred_element_type=jnp.float32
    )
    weight_grad = weight_grad - lax.dot_general(
        reconstructed_ratings, negative_group, contract, preferred_element_type=jnp.float32
    )
    visible_grad = jnp.sum(shown.astype(jnp.float32), axis=0) - jnp.sum(
        reconstructed_ratings.astype(jnp.float32), axis=0
    )
    weight_grad, visible_grad = lax.psum((weight_grad, visible_grad), "user")
    hidden_grad = lax.psum(jnp.sum(positive_own - negative_own, axis=0), ("movie", "user"))
    return (
        weight_grad.reshape(levels, local_movies, hidden),
        visible_grad.reshape(levels, local_movies),
        hidden_grad,
        positive_own,
    )


def solution(mesh):
    in_specs = (
        P(("movie", "user"), None),
        P(("movie", "user"), None),
        P(("movie", "user"), None),
        P(None, "movie", None),
        P(None, "movie"),
        P(),
    )
    out_specs = (P(None, "movie", None), P(None, "movie"), P(), P(("movie", "user"), None))

    def step(movie_ids, ratings, valid, weights, vis_bias, hid_bias):
        owners = mesh.shape["movie"]
        local_users = movie_ids.shape[0] // (owners * mesh.shape["user"])
        levels, movies, hidden = weights.shape
        fits = fits_kernels(mesh, local_users, movie_ids.shape[1], levels, movies // owners, hidden)
        return jax.shard_map(
            on_device_kernels if fits else on_device,
            mesh=mesh,
            in_specs=in_specs,
            out_specs=out_specs,
            check_vma=False,
        )(movie_ids, ratings, valid, weights, vis_bias, hid_bias)

    return step
```

```python
import functools

import jax
import jax.numpy as jnp
from jax import lax
from jax.experimental import pallas as pl
from jax.experimental.pallas import tpu as pltpu
from jax.sharding import PartitionSpec as P

LANES = 128
F32 = jnp.float32
BF16 = jnp.bfloat16
MIB = 1 << 20
TILES = (7, 5, 4, 10)
PARTS = (2, 4, 5, 7)
WIDE_TILE = 256
TN = (((0,), (0,)), ((), ()))
NT = (((1,), (1,)), ((), ()))


def positive_kernel(codes_ref, source, partial_ref, rating_ref, head, table, shown, movie_s, grade_s, total, arrived):
    sources, local_users, slots = codes_ref.shape
    half = slots // 2
    local_movies = rating_ref.shape[0]
    levels = source.shape[0] // local_movies
    tile = head.shape[0] // levels
    rest = local_movies - tile
    blocks = [(0, levels * tile, head, 0)]
    blocks += [(levels * tile + k * rest, rest, table, k * rest) for k in range(levels)]
    copies = []
    for k in range(levels):
        first = k * local_movies
        copies.append((source.at[pl.ds(first, tile)], head.at[pl.ds(k * tile, tile)]))
    for k in range(levels):
        first = k * local_movies + tile
        copies.append((source.at[pl.ds(first, rest)], table.at[pl.ds(k * rest, rest)]))
    copies = [pltpu.make_async_copy(*pair, arrived.at[i]) for i, pair in enumerate(copies)]
    for copy in copies:
        copy.start()

    rows = jnp.concatenate([codes_ref[i] for i in range(sources)], axis=0).astype(F32)
    turned = rows.T
    both = jnp.concatenate([turned[:half], turned[half:]], axis=1)
    movie = jnp.floor(both * 0.125)
    movie_s[...] = movie - (lax.axis_index("movie") * local_movies).astype(F32)
    grade_s[...] = both - movie * 8.0
    place = lax.broadcasted_iota(jnp.int32, (tile, LANES), 0).astype(F32).astype(BF16)

    for at in range(0, local_movies, tile):

        def add_slot(slot, found):
            movie = jnp.broadcast_to(movie_s[pl.ds(slot, 1), :] - float(at), (16, LANES)).astype(BF16)
            grade = jnp.broadcast_to(grade_s[pl.ds(slot, 1), :], (16, LANES)).astype(BF16)
            movie = jnp.tile(movie, (tile // 16, 1))
            grade = jnp.tile(grade, (tile // 16, 1))
            return jnp.where(place == movie, grade, found)

        found = lax.fori_loop(0, half, add_slot, jnp.full((tile, LANES), -1.0, BF16), unroll=16)
        wide = found.astype(F32)
        wide = jnp.maximum(wide, pltpu.roll(wide, LANES // 2, 1))
        rating_ref[at : at + tile, :] = wide.astype(BF16)
        for k in range(levels):
            first = k * tile if at == 0 else levels * tile + k * rest + at - tile
            shown[first : first + tile, :] = jnp.where(wide == float(k), 1.0, 0.0).astype(BF16)

    waits = [copies[:levels]] + [[copy] for copy in copies[levels:]]
    for i, (at, size, ref, start) in enumerate(blocks):
        for copy in waits[i]:
            copy.wait()
        part = lax.dot_general(
            shown[at : at + size, :], ref[start : start + size, :], TN, preferred_element_type=F32
        )
        total[...] = part if i == 0 else total[...] + part
    for i in range(sources):
        partial_ref[i] = total[i * local_users : (i + 1) * local_users, :].astype(partial_ref.dtype)


def negative_kernel(rows_ref, source, head, bias_ref, rating_ref, own_ref, partial_ref, stats_ref, own_out, table, probs, bias_s, total, arrived, sent):
    sources, local_users, hidden = rows_ref.shape
    users = sources * local_users
    local_movies = rating_ref.shape[0]
    levels = source.shape[0] // local_movies
    held = head.shape[0] // levels
    tiles = movie_tiles(held, local_movies)
    copies = [[]] + [
        [
            pltpu.make_async_copy(
                source.at[pl.ds(k * local_movies + at, tile)],
                table.at[pl.ds(levels * (at - held) + k * tile, tile)],
                arrived.at[t, k],
            )
            for k in range(levels)
        ]
        for t, (at, tile) in enumerate(tiles[1:])
    ]
    for group in copies:
        for copy in group:
            copy.start()

    own_copy = pltpu.make_async_copy(own_ref, own_out, sent)
    own_copy.start()
    spare = jnp.zeros((8 - levels, local_movies), F32)
    bias_s[...] = jnp.concatenate([bias_ref[...], spare], axis=0).T
    rows = jnp.concatenate([rows_ref[i].astype(F32) for i in range(sources)], axis=0)
    probs[...] = jnp.concatenate([rows, rows], axis=0).T.astype(BF16)
    def block(t):
        at, tile = tiles[t]
        return head[...] if t == 0 else table[levels * (at - held) : levels * (at - held + tile), :]

    def logits(t):
        for copy in copies[t]:
            copy.wait()
        return jnp.dot(block(t), probs[...], preferred_element_type=F32)

    ready = logits(0)
    for t, (start, tile) in enumerate(tiles):
        following = logits(t + 1) if t < len(tiles) - 1 else None
        first = lax.broadcasted_iota(jnp.int32, (tile, LANES), 1) < LANES // 2
        own = slice(start, start + tile)
        bias = bias_s[own, :]
        level = [ready[k * tile : (k + 1) * tile] + bias[:, k : k + 1] for k in range(levels)]
        largest = functools.reduce(jnp.maximum, level)
        level = [jnp.exp(x - largest) for x in level]
        scale = 1.0 / functools.reduce(jnp.add, level)
        rating = rating_ref[own, :].astype(F32)
        scale = jnp.where(rating >= 0.0, scale, 0.0)
        stats = []
        for k in range(levels):
            shown = jnp.where(rating == float(k), 1.0, 0.0)
            stats.append(jnp.where(first, shown, -(level[k] * scale)).astype(BF16))
            at = k * local_movies + start
            stats_ref[at : at + tile, :] = stats[k]
        stats = jnp.concatenate(stats, axis=0)
        part = lax.dot_general(
            stats, block(t), TN, preferred_element_type=F32
        )
        total[...] = part if t == 0 else total[...] + part
        ready = following
    for i in range(sources):
        row = users + i * local_users
        partial_ref[i] = (-total[row : row + local_users, :]).astype(partial_ref.dtype)
    own_copy.wait()


def positive_rows_kernel(parts_ref, bias_ref, own_ref, sent_ref):
    sources = parts_ref.shape[0]
    summed = functools.reduce(jnp.add, [parts_ref[i].astype(F32) for i in range(sources)])
    own = jax.nn.sigmoid(bias_ref[...] + summed)
    own_ref[...] = own
    low = own.astype(BF16)
    for i in range(sources):
        sent_ref[i] = low


def negative_rows_kernel(parts_ref, bias_ref, positive_ref, sent_ref):
    sources, local_users, hidden = parts_ref.shape
    side = hidden // local_users
    summed = functools.reduce(jnp.add, [parts_ref[i].astype(F32) for i in range(sources)])
    own = jax.nn.sigmoid(bias_ref[...] + summed)
    positive = positive_ref[...]
    lost = (positive - positive.astype(BF16).astype(F32)) - (own - own.astype(BF16).astype(F32))
    lost = jnp.sum(lost, axis=0, keepdims=True)
    split = [lost[:, i * side : (i + 1) * side] for i in range(local_users)]
    low = jnp.concatenate([own, jnp.concatenate(split, axis=0)], axis=1).astype(BF16)
    for i in range(sources):
        sent_ref[i] = low


def gathered_rows_kernel(pos_ref, neg_ref, rows_ref):
    sources, _, hidden = pos_ref.shape
    wide = [neg_ref[i].astype(F32) for i in range(sources)]
    block = [pos_ref[i].astype(F32) for i in range(sources)] + [x[:, :hidden] for x in wide]
    sides = functools.reduce(jnp.add, [x[:, hidden:] for x in wide])
    rest = jnp.concatenate([sides[i : i + 1] for i in range(sides.shape[0])], axis=1)
    terms = []
    for _ in range(3):
        terms.append(rest.astype(BF16).astype(F32))
        rest = rest - terms[-1]
    spare = jnp.zeros((rows_ref.shape[0] - LANES - len(terms), hidden), F32)
    rows_ref[...] = jnp.concatenate(block + terms + [spare], axis=0).astype(BF16)


def halves():
    mine = pl.multiple_of(lax.axis_index("user") * LANES, LANES)
    return mine, pl.multiple_of(LANES - mine, LANES)


def first_level_kernel(stats_a, stats_b, lhs_ref, other_s, arrived):
    mine, other = halves()
    copy = pltpu.make_async_copy(stats_b.at[0], other_s, arrived)
    copy.start()
    lhs_ref[:, pl.ds(mine, LANES)] = stats_a[0]
    copy.wait()
    lhs_ref[:, pl.ds(other, LANES)] = other_s[...]


def gradient_kernel(stats_a, stats_b, first, rows_a, rows_b, target, visible_out, hidden_out, stats_s, visible_ref, hidden_ref, lhs, rhs, slots, sent, got, done):
    levels, local_movies, _ = stats_a.shape
    buffers, rows, _ = slots.shape
    parts = local_movies // rows
    mine, other = halves()

    fetch = [pltpu.make_async_copy(stats_b.at[i], stats_s.at[i], got.at[i]) for i in range(1, levels)]
    for copy in fetch:
        copy.start()
    rhs[pl.ds(mine, LANES), :] = rows_a[:LANES, :]
    rhs[pl.ds(other, LANES), :] = rows_b[:LANES, :]
    lhs[...] = first[...]
    ones = jnp.ones((8, 2 * LANES), BF16)

    def send(level, part, slot):
        place = target.at[level, pl.ds(part * rows, rows)]
        return pltpu.make_async_copy(slots.at[slot], place, sent.at[slot])

    def one_level(level, carry):
        @pl.when(level > 0)
        def _():
            pltpu.make_async_copy(stats_b.at[level], stats_s.at[level], got.at[level]).wait()
            lhs[:, pl.ds(mine, LANES)] = stats_a[level]
            lhs[:, pl.ds(other, LANES)] = stats_s[level]

        for part in range(parts):
            count = level * parts + part
            slot = lax.rem(count, buffers)

            @pl.when(count >= buffers)
            def _():
                send(level, part, slot).wait()

            block = lhs[part * rows : (part + 1) * rows, :]
            slots[slot] = jnp.dot(block, rhs[...], preferred_element_type=F32)
            send(level, part, slot).start()
        summed = lax.dot_general(ones, lhs[...], NT, preferred_element_type=F32)
        visible_ref[pl.ds(level, 1), :] = summed[:1]
        return carry

    lax.fori_loop(0, levels, one_level, 0)

    def total(ref, first, last):
        return jnp.sum(ref[first:last, :].astype(F32), axis=0, keepdims=True)

    users = LANES // 2
    sums = [
        total(ref, 0, users) - total(ref, users, LANES) + total(ref, LANES, LANES + 16) for ref in (rows_a, rows_b)
    ]
    hidden_ref[...] = sums[0] + sums[1]
    small = [
        pltpu.make_async_copy(visible_ref, visible_out, done.at[0]),
        pltpu.make_async_copy(hidden_ref, hidden_out, done.at[1]),
    ]
    for copy in small:
        copy.start()
    for slot in range(min(buffers, levels * parts)):
        send(0, 0, slot).wait()
    for copy in small:
        copy.wait()


def whole(shape):
    return pl.BlockSpec(shape, lambda *_: (0,) * len(shape))


def params(limit):
    return pltpu.CompilerParams(vmem_limit_bytes=limit)


def exchange(x):
    return lax.all_to_all(x, "movie", split_axis=0, concat_axis=0, tiled=True)


def pick_tile(local_movies, parts):
    for count in parts:
        if local_movies % count == 0 and (local_movies // count) % 16 == 0:
            return local_movies // count
    return None


def movie_tiles(held, movies):
    wide, left = divmod(movies - held, WIDE_TILE)
    edge = left // 2 if left % 32 == 0 else left
    sizes = [held, edge] + [WIDE_TILE] * wide + [left - edge]
    sizes = [size for size in sizes if size]
    return [(sum(sizes[:i]), size) for i, size in enumerate(sizes)]


def on_device_kernels(movie_ids, ratings, valid, weights, vis_bias, hid_bias):
    owners = lax.axis_size("movie")
    local_users, slots = movie_ids.shape
    levels, local_movies, hidden = weights.shape
    columns = levels * local_movies
    users = owners * local_users
    tile = pick_tile(local_movies, TILES)
    part = pick_tile(local_movies, PARTS)
    swap = [(0, 1), (1, 0)]
    matmul = 2 * users * columns * hidden
    table_bytes = weights.size * 2

    code = jnp.where(valid == 1, movie_ids * 8 + ratings, -8)
    codes = exchange(jnp.broadcast_to(code[None], (owners, local_users, slots)))
    table = pltpu.with_memory_space_constraint(weights.reshape(columns, hidden), pltpu.HBM)
    bias_row = hid_bias[None, :]
    table_scratch = pltpu.VMEM((levels * (local_movies - tile), hidden), BF16)
    total_scratch = pltpu.VMEM((LANES, hidden), F32)
    vmem = pl.BlockSpec(memory_space=pltpu.VMEM)
    table_spec = pl.BlockSpec(memory_space=pltpu.HBM)
    parts_shape = (owners, local_users, hidden)

    positive_part, rating, head = pl.pallas_call(
        positive_kernel,
        in_specs=[vmem, table_spec],
        out_specs=[vmem, vmem, vmem],
        out_shape=[
            pltpu.VMEM(parts_shape, F32),
            jax.ShapeDtypeStruct((local_movies, LANES), BF16),
            pltpu.VMEM((levels * tile, hidden), BF16),
        ],
        scratch_shapes=[
            table_scratch,
            pltpu.VMEM((columns, LANES), BF16),
            pltpu.VMEM((slots // 2, LANES), F32),
            pltpu.VMEM((slots // 2, LANES), F32),
            total_scratch,
            pltpu.SemaphoreType.DMA((2 * levels,)),
        ],
        compiler_params=params(32 * MIB),
        cost_estimate=pl.CostEstimate(flops=matmul, bytes_accessed=table_bytes, transcendentals=0),
        name="positive",
    )(codes, table)

    positive_own, sent = pl.pallas_call(
        positive_rows_kernel,
        out_shape=[
            pltpu.VMEM((local_users, hidden), F32),
            pltpu.VMEM(parts_shape, BF16),
        ],
        compiler_params=params(8 * MIB),
        name="positive_rows",
    )(exchange(positive_part), bias_row)
    pos_a = exchange(sent)

    negative_part, stats_a, positive_out = pl.pallas_call(
        negative_kernel,
        in_specs=[vmem, table_spec, vmem, vmem, vmem, vmem],
        out_specs=[vmem, vmem, pl.BlockSpec(memory_space=pltpu.HBM)],
        out_shape=[
            pltpu.VMEM(parts_shape, BF16),
            jax.ShapeDtypeStruct((columns, LANES), BF16),
            jax.ShapeDtypeStruct(positive_own.shape, F32),
        ],
        scratch_shapes=[
            table_scratch,
            pltpu.VMEM((hidden, LANES), BF16),
            pltpu.VMEM((local_movies, 8), F32),
            total_scratch,
            pltpu.SemaphoreType.DMA((len(movie_tiles(tile, local_movies)), levels)),
            pltpu.SemaphoreType.DMA,
        ],
        compiler_params=params(32 * MIB),
        cost_estimate=pl.CostEstimate(flops=2 * matmul, bytes_accessed=table_bytes, transcendentals=0),
        name="negative",
    )(pos_a, table, head, vis_bias, rating, positive_own)
    stats_a = stats_a.reshape(levels, local_movies, LANES)
    stats_b = lax.ppermute(stats_a, "user", swap)

    sent = pl.pallas_call(
        negative_rows_kernel,
        out_shape=pltpu.VMEM((owners, local_users, hidden + hidden // local_users), BF16),
        compiler_params=params(8 * MIB),
        name="negative_rows",
    )(exchange(negative_part), bias_row, positive_own)
    rows_a = pl.pallas_call(
        gathered_rows_kernel,
        out_shape=pltpu.VMEM((LANES + 16, hidden), BF16),
        compiler_params=params(8 * MIB),
        name="gathered_rows",
    )(pos_a, exchange(sent))
    rows_b = lax.ppermute(rows_a, "user", swap)
    first = pl.pallas_call(
        first_level_kernel,
        in_specs=[vmem, pl.BlockSpec(memory_space=pl.ANY)],
        out_specs=vmem,
        out_shape=pltpu.VMEM((local_movies, 2 * LANES), BF16),
        scratch_shapes=[pltpu.VMEM((local_movies, LANES), BF16), pltpu.SemaphoreType.DMA],
        compiler_params=params(8 * MIB),
        cost_estimate=pl.CostEstimate(flops=1 << 27, bytes_accessed=1 << 20, transcendentals=0),
        name="first_level",
    )(stats_a, stats_b)
    weight_grad, visible_grad, hidden_grad = pl.pallas_call(
        gradient_kernel,
        in_specs=[vmem, pl.BlockSpec(memory_space=pl.ANY)] + [vmem] * 3,
        out_specs=[pl.BlockSpec(memory_space=pltpu.HBM)] * 3,
        out_shape=[
            jax.ShapeDtypeStruct(weights.shape, F32),
            jax.ShapeDtypeStruct((levels, local_movies), F32),
            jax.ShapeDtypeStruct((1, hidden), F32),
        ],
        scratch_shapes=[
            pltpu.VMEM(stats_a.shape, BF16),
            pltpu.VMEM((levels, local_movies), F32),
            pltpu.VMEM((1, hidden), F32),
            pltpu.VMEM((local_movies, 2 * LANES), BF16),
            pltpu.VMEM((2 * LANES, hidden), BF16),
            pltpu.VMEM((3, part, hidden), F32),
            pltpu.SemaphoreType.DMA((3,)),
            pltpu.SemaphoreType.DMA((levels,)),
            pltpu.SemaphoreType.DMA((2,)),
        ],
        compiler_params=params(32 * MIB),
        cost_estimate=pl.CostEstimate(flops=4 * matmul, bytes_accessed=2 * table_bytes, transcendentals=0),
        name="gradient",
    )(stats_a, stats_b, first, rows_a, rows_b)
    return weight_grad, visible_grad, hidden_grad[0], positive_out


def fits_kernels(mesh, local_users, slots, levels, local_movies, hidden):
    users = mesh.shape["movie"] * local_users
    return (
        mesh.shape["user"] == 2
        and users == LANES // 2
        and slots % 16 == 0
        and hidden % (LANES * local_users) == 0
        and local_users == 4
        and levels < 8
        and pick_tile(local_movies, TILES) is not None
        and pick_tile(local_movies, PARTS) is not None
    )


def reconstruct(hidden_rows, weight_table, bias_row, rated_mask, levels):
    group_rows = hidden_rows.shape[0]
    rating_logits = (
        lax.dot_general(
            hidden_rows, weight_table, (((1,), (1,)), ((), ())), preferred_element_type=jnp.float32
        )
        + bias_row[None, :]
    )
    shaped = rating_logits.reshape(group_rows, levels, -1)
    largest = jnp.max(shaped, axis=1, keepdims=True)
    exponent = jnp.exp(shaped - largest)
    softened = (exponent / jnp.sum(exponent, axis=1, keepdims=True)).astype(jnp.bfloat16)
    return (softened * rated_mask[:, None, :]).reshape(group_rows, -1)


def hidden_phase(visible, weight_table, hid_bias, local_users, device_index):
    combined = jnp.dot(visible, weight_table, preferred_element_type=jnp.float32)
    all_probs = jax.nn.sigmoid(hid_bias[None, :] + lax.psum(combined, "movie"))
    own_rows = lax.dynamic_slice_in_dim(all_probs, device_index * local_users, local_users, 0)
    return (own_rows, all_probs.astype(jnp.bfloat16))


def on_device(movie_ids, ratings, valid, weights, vis_bias, hid_bias):
    owners = lax.axis_size("movie")
    device_index = lax.axis_index("movie")
    local_users, slot_count = movie_ids.shape
    levels, local_movies, hidden = weights.shape
    columns = levels * local_movies
    group_rows = owners * local_users
    capacity = max(2, 3 * local_users * slot_count // owners)
    flat_ids = movie_ids.reshape(-1)
    owner_ids = flat_ids // local_movies
    column_ids = ratings.reshape(-1) * local_movies + flat_ids % local_movies
    user_ids = jnp.arange(local_users * slot_count, dtype=jnp.int32) // slot_count
    usable = valid.reshape(-1) == 1
    matches = (owner_ids[:, None] == jnp.arange(owners, dtype=jnp.int32)[None, :]) & usable[:, None]
    ranking = jnp.cumsum(matches.astype(jnp.int32), axis=0) - 1
    placed = jnp.sum(jnp.where(matches, ranking, 0), axis=1)
    target = jnp.where(usable, owner_ids, owners)
    user_slots = (
        jnp.zeros((owners, capacity), jnp.int32).at[target, placed].set(user_ids, mode="drop")
    )
    column_slots = (
        jnp.full((owners, capacity), -1, jnp.int32).at[target, placed].set(column_ids, mode="drop")
    )
    got_users, got_columns = (
        lax.all_to_all(user_slots, "movie", split_axis=0, concat_axis=0, tiled=True),
        lax.all_to_all(column_slots, "movie", split_axis=0, concat_axis=0, tiled=True),
    )
    user_hot = (got_users[:, :, None] == jnp.arange(local_users, dtype=jnp.int32)).astype(
        jnp.bfloat16
    )
    column_hot = (got_columns[:, :, None] == jnp.arange(columns, dtype=jnp.int32)).astype(
        jnp.bfloat16
    )
    shown = jnp.einsum("ncu,ncj->nuj", user_hot, column_hot, preferred_element_type=jnp.float32)
    shown = shown.reshape(group_rows, columns).astype(jnp.bfloat16)
    rated_mask = jnp.sum(shown.reshape(group_rows, levels, local_movies), axis=1)
    weight_table = weights.reshape(columns, hidden)
    positive_own, positive_group = hidden_phase(
        shown, weight_table, hid_bias, local_users, device_index
    )
    reconstructed_ratings = reconstruct(
        positive_group, weight_table, vis_bias.reshape(columns), rated_mask, levels
    )
    negative_own, negative_group = hidden_phase(
        reconstructed_ratings, weight_table, hid_bias, local_users, device_index
    )
    contract = (((0,), (0,)), ((), ()))
    weight_grad = lax.dot_general(
        shown, positive_group, contract, preferred_element_type=jnp.float32
    )
    weight_grad = weight_grad - lax.dot_general(
        reconstructed_ratings, negative_group, contract, preferred_element_type=jnp.float32
    )
    visible_grad = jnp.sum(shown.astype(jnp.float32), axis=0) - jnp.sum(
        reconstructed_ratings.astype(jnp.float32), axis=0
    )
    weight_grad, visible_grad = lax.psum((weight_grad, visible_grad), "user")
    hidden_grad = lax.psum(jnp.sum(positive_own - negative_own, axis=0), ("movie", "user"))
    return (
        weight_grad.reshape(levels, local_movies, hidden),
        visible_grad.reshape(levels, local_movies),
        hidden_grad,
        positive_own,
    )


def solution(mesh):
    in_specs = (
        P(("movie", "user"), None),
        P(("movie", "user"), None),
        P(("movie", "user"), None),
        P(None, "movie", None),
        P(None, "movie"),
        P(),
    )
    out_specs = (P(None, "movie", None), P(None, "movie"), P(), P(("movie", "user"), None))

    def step(movie_ids, ratings, valid, weights, vis_bias, hid_bias):
        owners = mesh.shape["movie"]
        local_users = movie_ids.shape[0] // (owners * mesh.shape["user"])
        levels, movies, hidden = weights.shape
        fits = fits_kernels(mesh, local_users, movie_ids.shape[1], levels, movies // owners, hidden)
        return jax.shard_map(
            on_device_kernels if fits else on_device,
            mesh=mesh,
            in_specs=in_specs,
            out_specs=out_specs,
            check_vma=False,
        )(movie_ids, ratings, valid, weights, vis_bias, hid_bias)

    return step
```

```python
import functools

import jax
import jax.numpy as jnp
from jax import lax
from jax.experimental import pallas as pl
from jax.experimental.pallas import tpu as pltpu
from jax.sharding import PartitionSpec as P

LANES = 128
F32 = jnp.float32
BF16 = jnp.bfloat16
MIB = 1 << 20
TILES = (7, 5, 4, 10)
PARTS = (2, 4, 5, 7)
WIDE_TILE = 256
TN = (((0,), (0,)), ((), ()))
NT = (((1,), (1,)), ((), ()))


def positive_kernel(codes_ref, source, partial_ref, rating_ref, head, table, shown, movie_s, grade_s, total, arrived):
    sources, local_users, slots = codes_ref.shape
    half = slots // 2
    local_movies = rating_ref.shape[0]
    levels = source.shape[0] // local_movies
    tile = head.shape[0] // levels
    rest = local_movies - tile
    blocks = [(0, levels * tile, head, 0)]
    last = min(WIDE_TILE, rest // 2)
    runs = [(k * rest, rest) for k in range(levels - 1)]
    runs += [((levels - 1) * rest, rest - last), (levels * rest - last, last)]
    blocks += [(levels * tile + at, size, table, at) for at, size in runs]
    copies = []
    for k in range(levels):
        first = k * local_movies
        copies.append((source.at[pl.ds(first, tile)], head.at[pl.ds(k * tile, tile)]))
    for at, size in runs:
        first = at + tile * (at // rest + 1)
        copies.append((source.at[pl.ds(first, size)], table.at[pl.ds(at, size)]))
    copies = [pltpu.make_async_copy(*pair, arrived.at[i]) for i, pair in enumerate(copies)]
    for copy in copies:
        copy.start()

    rows = jnp.concatenate([codes_ref[i] for i in range(sources)], axis=0).astype(F32)
    turned = rows.T
    both = jnp.concatenate([turned[:half], turned[half:]], axis=1)
    movie = jnp.floor(both * 0.125)
    movie_s[...] = movie - (lax.axis_index("movie") * local_movies).astype(F32)
    grade_s[...] = both - movie * 8.0
    place = lax.broadcasted_iota(jnp.int32, (tile, LANES), 0).astype(F32).astype(BF16)

    for at in range(0, local_movies, tile):

        def add_slot(slot, found):
            movie = jnp.broadcast_to(movie_s[pl.ds(slot, 1), :] - float(at), (16, LANES)).astype(BF16)
            grade = jnp.broadcast_to(grade_s[pl.ds(slot, 1), :], (16, LANES)).astype(BF16)
            movie = jnp.tile(movie, (tile // 16, 1))
            grade = jnp.tile(grade, (tile // 16, 1))
            return jnp.where(place == movie, grade, found)

        found = lax.fori_loop(0, half, add_slot, jnp.full((tile, LANES), -1.0, BF16), unroll=16)
        wide = found.astype(F32)
        wide = jnp.maximum(wide, pltpu.roll(wide, LANES // 2, 1))
        rating_ref[at : at + tile, :] = wide.astype(BF16)
        for k in range(levels):
            first = k * tile if at == 0 else levels * tile + k * rest + at - tile
            shown[first : first + tile, :] = jnp.where(wide == float(k), 1.0, 0.0).astype(BF16)

    waits = [copies[:levels]] + [[copy] for copy in copies[levels:]]
    for i, (at, size, ref, start) in enumerate(blocks):
        for copy in waits[i]:
            copy.wait()
        part = lax.dot_general(
            shown[at : at + size, :], ref[start : start + size, :], TN, preferred_element_type=F32
        )
        total[...] = part if i == 0 else total[...] + part
    for i in range(sources):
        partial_ref[i] = total[i * local_users : (i + 1) * local_users, :].astype(partial_ref.dtype)


def negative_kernel(rows_ref, source, head, bias_ref, rating_ref, own_ref, partial_ref, stats_ref, own_out, table, probs, bias_s, total, arrived, sent):
    sources, local_users, hidden = rows_ref.shape
    users = sources * local_users
    local_movies = rating_ref.shape[0]
    levels = source.shape[0] // local_movies
    held = head.shape[0] // levels
    tiles = movie_tiles(held, local_movies)
    copies = [[]] + [
        [
            pltpu.make_async_copy(
                source.at[pl.ds(k * local_movies + at, tile)],
                table.at[pl.ds(levels * (at - held) + k * tile, tile)],
                arrived.at[t, k],
            )
            for k in range(levels)
        ]
        for t, (at, tile) in enumerate(tiles[1:])
    ]
    for group in copies:
        for copy in group:
            copy.start()

    own_copy = pltpu.make_async_copy(own_ref, own_out, sent)
    own_copy.start()
    spare = jnp.zeros((8 - levels, local_movies), F32)
    bias_s[...] = jnp.concatenate([bias_ref[...], spare], axis=0).T
    rows = jnp.concatenate([rows_ref[i].astype(F32) for i in range(sources)], axis=0)
    probs[...] = jnp.concatenate([rows, rows], axis=0).T.astype(BF16)
    def block(t):
        at, tile = tiles[t]
        return head[...] if t == 0 else table[levels * (at - held) : levels * (at - held + tile), :]

    def logits(t):
        for copy in copies[t]:
            copy.wait()
        return jnp.dot(block(t), probs[...], preferred_element_type=F32)

    ready = logits(0)
    for t, (start, tile) in enumerate(tiles):
        following = logits(t + 1) if t < len(tiles) - 1 else None
        first = lax.broadcasted_iota(jnp.int32, (tile, LANES), 1) < LANES // 2
        own = slice(start, start + tile)
        bias = bias_s[own, :]
        level = [ready[k * tile : (k + 1) * tile] + bias[:, k : k + 1] for k in range(levels)]
        largest = functools.reduce(jnp.maximum, level)
        level = [jnp.exp(x - largest) for x in level]
        scale = 1.0 / functools.reduce(jnp.add, level)
        rating = rating_ref[own, :].astype(F32)
        scale = jnp.where(rating >= 0.0, scale, 0.0)
        stats = []
        for k in range(levels):
            shown = jnp.where(rating == float(k), 1.0, 0.0)
            stats.append(jnp.where(first, shown, -(level[k] * scale)).astype(BF16))
            at = k * local_movies + start
            stats_ref[at : at + tile, :] = stats[k]
        stats = jnp.concatenate(stats, axis=0)
        part = lax.dot_general(
            stats, block(t), TN, preferred_element_type=F32
        )
        total[...] = part if t == 0 else total[...] + part
        ready = following
    for i in range(sources):
        row = users + i * local_users
        partial_ref[i] = (-total[row : row + local_users, :]).astype(partial_ref.dtype)
    own_copy.wait()


def positive_rows_kernel(parts_ref, bias_ref, own_ref, sent_ref):
    sources = parts_ref.shape[0]
    summed = functools.reduce(jnp.add, [parts_ref[i].astype(F32) for i in range(sources)])
    own = jax.nn.sigmoid(bias_ref[...] + summed)
    own_ref[...] = own
    low = own.astype(BF16)
    for i in range(sources):
        sent_ref[i] = low


def negative_rows_kernel(parts_ref, bias_ref, positive_ref, sent_ref):
    sources, local_users, hidden = parts_ref.shape
    side = hidden // local_users
    summed = functools.reduce(jnp.add, [parts_ref[i].astype(F32) for i in range(sources)])
    own = jax.nn.sigmoid(bias_ref[...] + summed)
    positive = positive_ref[...]
    lost = (positive - positive.astype(BF16).astype(F32)) - (own - own.astype(BF16).astype(F32))
    lost = jnp.sum(lost, axis=0, keepdims=True)
    split = [lost[:, i * side : (i + 1) * side] for i in range(local_users)]
    low = jnp.concatenate([own, jnp.concatenate(split, axis=0)], axis=1).astype(BF16)
    for i in range(sources):
        sent_ref[i] = low


def gathered_rows_kernel(pos_ref, neg_ref, rows_ref):
    sources, _, hidden = pos_ref.shape
    wide = [neg_ref[i].astype(F32) for i in range(sources)]
    block = [pos_ref[i].astype(F32) for i in range(sources)] + [x[:, :hidden] for x in wide]
    sides = functools.reduce(jnp.add, [x[:, hidden:] for x in wide])
    rest = jnp.concatenate([sides[i : i + 1] for i in range(sides.shape[0])], axis=1)
    terms = []
    for _ in range(3):
        terms.append(rest.astype(BF16).astype(F32))
        rest = rest - terms[-1]
    spare = jnp.zeros((rows_ref.shape[0] - LANES - len(terms), hidden), F32)
    rows_ref[...] = jnp.concatenate(block + terms + [spare], axis=0).astype(BF16)


def halves():
    mine = pl.multiple_of(lax.axis_index("user") * LANES, LANES)
    return mine, pl.multiple_of(LANES - mine, LANES)


def first_level_kernel(stats_a, stats_b, lhs_ref, other_s, arrived):
    mine, other = halves()
    copy = pltpu.make_async_copy(stats_b.at[0], other_s, arrived)
    copy.start()
    lhs_ref[:, pl.ds(mine, LANES)] = stats_a[0]
    copy.wait()
    lhs_ref[:, pl.ds(other, LANES)] = other_s[...]


def gradient_kernel(stats_a, stats_b, first, rows_a, rows_b, target, visible_out, hidden_out, stats_s, visible_ref, hidden_ref, lhs, rhs, slots, sent, got, done):
    levels, local_movies, _ = stats_a.shape
    buffers, rows, _ = slots.shape
    parts = local_movies // rows
    mine, other = halves()

    fetch = [pltpu.make_async_copy(stats_b.at[i], stats_s.at[i], got.at[i]) for i in range(1, levels)]
    for copy in fetch:
        copy.start()
    rhs[pl.ds(mine, LANES), :] = rows_a[:LANES, :]
    rhs[pl.ds(other, LANES), :] = rows_b[:LANES, :]
    lhs[...] = first[...]
    ones = jnp.ones((8, 2 * LANES), BF16)

    def send(level, part, slot):
        place = target.at[level, pl.ds(part * rows, rows)]
        return pltpu.make_async_copy(slots.at[slot], place, sent.at[slot])

    def one_level(level, carry):
        if not isinstance(level, int):
            pltpu.make_async_copy(stats_b.at[level], stats_s.at[level], got.at[level]).wait()
            lhs[:, pl.ds(mine, LANES)] = stats_a[level]
            lhs[:, pl.ds(other, LANES)] = stats_s[level]

        for part in range(parts):
            count = level * parts + part
            slot = count % buffers if isinstance(count, int) else lax.rem(count, buffers)
            if isinstance(count, int):
                if count >= buffers:
                    send(level, part, slot).wait()
            else:

                @pl.when(count >= buffers)
                def _():
                    send(level, part, slot).wait()

            edges = [0, rows]
            if isinstance(level, int) and part == 0 and rows > 2 * LANES:
                edges = [0, LANES, rows]
            for low, high in zip(edges, edges[1:]):
                block = lhs[part * rows + low : part * rows + high, :]
                slots[slot, low:high] = jnp.dot(block, rhs[...], preferred_element_type=F32)
                place = target.at[level, pl.ds(part * rows + low, high - low)]
                pltpu.make_async_copy(slots.at[slot, pl.ds(low, high - low)], place, sent.at[slot]).start()
        summed = lax.dot_general(ones, lhs[...], NT, preferred_element_type=F32)
        visible_ref[pl.ds(level, 1), :] = summed[:1]
        return carry

    one_level(0, 0)
    lax.fori_loop(1, levels, one_level, 0)

    def total(ref, first, last):
        return jnp.sum(ref[first:last, :].astype(F32), axis=0, keepdims=True)

    users = LANES // 2
    sums = [
        total(ref, 0, users) - total(ref, users, LANES) + total(ref, LANES, LANES + 16) for ref in (rows_a, rows_b)
    ]
    hidden_ref[...] = sums[0] + sums[1]
    small = [
        pltpu.make_async_copy(visible_ref, visible_out, done.at[0]),
        pltpu.make_async_copy(hidden_ref, hidden_out, done.at[1]),
    ]
    for copy in small:
        copy.start()
    for slot in range(min(buffers, levels * parts)):
        send(0, 0, slot).wait()
    for copy in small:
        copy.wait()


def whole(shape):
    return pl.BlockSpec(shape, lambda *_: (0,) * len(shape))


def params(limit):
    return pltpu.CompilerParams(vmem_limit_bytes=limit)


def exchange(x):
    return lax.all_to_all(x, "movie", split_axis=0, concat_axis=0, tiled=True)


def pick_tile(local_movies, parts):
    for count in parts:
        if local_movies % count == 0 and (local_movies // count) % 16 == 0:
            return local_movies // count
    return None


def movie_tiles(held, movies):
    wide, left = divmod(movies - held, WIDE_TILE)
    edge = left // 2 if left % 32 == 0 else left
    sizes = [held, edge] + [WIDE_TILE] * wide + [left - edge]
    sizes = [size for size in sizes if size]
    return [(sum(sizes[:i]), size) for i, size in enumerate(sizes)]


def on_device_kernels(movie_ids, ratings, valid, weights, vis_bias, hid_bias):
    owners = lax.axis_size("movie")
    local_users, slots = movie_ids.shape
    levels, local_movies, hidden = weights.shape
    columns = levels * local_movies
    users = owners * local_users
    tile = pick_tile(local_movies, TILES)
    part = pick_tile(local_movies, PARTS)
    swap = [(0, 1), (1, 0)]
    matmul = 2 * users * columns * hidden
    table_bytes = weights.size * 2

    code = jnp.where(valid == 1, movie_ids * 8 + ratings, -8)
    codes = exchange(jnp.broadcast_to(code[None], (owners, local_users, slots)))
    table = pltpu.with_memory_space_constraint(weights.reshape(columns, hidden), pltpu.HBM)
    bias_row = hid_bias[None, :]
    table_scratch = pltpu.VMEM((levels * (local_movies - tile), hidden), BF16)
    total_scratch = pltpu.VMEM((LANES, hidden), F32)
    vmem = pl.BlockSpec(memory_space=pltpu.VMEM)
    table_spec = pl.BlockSpec(memory_space=pltpu.HBM)
    parts_shape = (owners, local_users, hidden)

    positive_part, rating, head = pl.pallas_call(
        positive_kernel,
        in_specs=[vmem, table_spec],
        out_specs=[vmem, vmem, vmem],
        out_shape=[
            pltpu.VMEM(parts_shape, F32),
            jax.ShapeDtypeStruct((local_movies, LANES), BF16),
            pltpu.VMEM((levels * tile, hidden), BF16),
        ],
        scratch_shapes=[
            table_scratch,
            pltpu.VMEM((columns, LANES), BF16),
            pltpu.VMEM((slots // 2, LANES), F32),
            pltpu.VMEM((slots // 2, LANES), F32),
            total_scratch,
            pltpu.SemaphoreType.DMA((2 * levels + 1,)),
        ],
        compiler_params=params(32 * MIB),
        cost_estimate=pl.CostEstimate(flops=matmul, bytes_accessed=table_bytes, transcendentals=0),
        name="positive",
    )(codes, table)

    positive_own, sent = pl.pallas_call(
        positive_rows_kernel,
        out_shape=[
            pltpu.VMEM((local_users, hidden), F32),
            pltpu.VMEM(parts_shape, BF16),
        ],
        compiler_params=params(8 * MIB),
        name="positive_rows",
    )(exchange(positive_part), bias_row)
    pos_a = exchange(sent)

    negative_part, stats_a, positive_out = pl.pallas_call(
        negative_kernel,
        in_specs=[vmem, table_spec, vmem, vmem, vmem, vmem],
        out_specs=[vmem, vmem, pl.BlockSpec(memory_space=pltpu.HBM)],
        out_shape=[
            pltpu.VMEM(parts_shape, BF16),
            jax.ShapeDtypeStruct((columns, LANES), BF16),
            jax.ShapeDtypeStruct(positive_own.shape, F32),
        ],
        scratch_shapes=[
            table_scratch,
            pltpu.VMEM((hidden, LANES), BF16),
            pltpu.VMEM((local_movies, 8), F32),
            total_scratch,
            pltpu.SemaphoreType.DMA((len(movie_tiles(tile, local_movies)), levels)),
            pltpu.SemaphoreType.DMA,
        ],
        compiler_params=params(32 * MIB),
        cost_estimate=pl.CostEstimate(flops=2 * matmul, bytes_accessed=table_bytes, transcendentals=0),
        name="negative",
    )(pos_a, table, head, vis_bias, rating, positive_own)
    stats_a = stats_a.reshape(levels, local_movies, LANES)
    stats_b = lax.ppermute(stats_a, "user", swap)

    sent = pl.pallas_call(
        negative_rows_kernel,
        out_shape=pltpu.VMEM((owners, local_users, hidden + hidden // local_users), BF16),
        compiler_params=params(8 * MIB),
        name="negative_rows",
    )(exchange(negative_part), bias_row, positive_own)
    rows_a = pl.pallas_call(
        gathered_rows_kernel,
        out_shape=pltpu.VMEM((LANES + 16, hidden), BF16),
        compiler_params=params(8 * MIB),
        name="gathered_rows",
    )(pos_a, exchange(sent))
    rows_b = lax.ppermute(rows_a, "user", swap)
    first = pl.pallas_call(
        first_level_kernel,
        in_specs=[vmem, pl.BlockSpec(memory_space=pl.ANY)],
        out_specs=vmem,
        out_shape=pltpu.VMEM((local_movies, 2 * LANES), BF16),
        scratch_shapes=[pltpu.VMEM((local_movies, LANES), BF16), pltpu.SemaphoreType.DMA],
        compiler_params=params(8 * MIB),
        cost_estimate=pl.CostEstimate(flops=1 << 27, bytes_accessed=1 << 20, transcendentals=0),
        name="first_level",
    )(stats_a, stats_b)
    weight_grad, visible_grad, hidden_grad = pl.pallas_call(
        gradient_kernel,
        in_specs=[vmem, pl.BlockSpec(memory_space=pl.ANY)] + [vmem] * 3,
        out_specs=[pl.BlockSpec(memory_space=pltpu.HBM)] * 3,
        out_shape=[
            jax.ShapeDtypeStruct(weights.shape, F32),
            jax.ShapeDtypeStruct((levels, local_movies), F32),
            jax.ShapeDtypeStruct((1, hidden), F32),
        ],
        scratch_shapes=[
            pltpu.VMEM(stats_a.shape, BF16),
            pltpu.VMEM((levels, local_movies), F32),
            pltpu.VMEM((1, hidden), F32),
            pltpu.VMEM((local_movies, 2 * LANES), BF16),
            pltpu.VMEM((2 * LANES, hidden), BF16),
            pltpu.VMEM((3, part, hidden), F32),
            pltpu.SemaphoreType.DMA((3,)),
            pltpu.SemaphoreType.DMA((levels,)),
            pltpu.SemaphoreType.DMA((2,)),
        ],
        compiler_params=params(32 * MIB),
        cost_estimate=pl.CostEstimate(flops=4 * matmul, bytes_accessed=2 * table_bytes, transcendentals=0),
        name="gradient",
    )(stats_a, stats_b, first, rows_a, rows_b)
    return weight_grad, visible_grad, hidden_grad[0], positive_out


def fits_kernels(mesh, local_users, slots, levels, local_movies, hidden):
    users = mesh.shape["movie"] * local_users
    return (
        mesh.shape["user"] == 2
        and users == LANES // 2
        and slots % 16 == 0
        and hidden % (LANES * local_users) == 0
        and local_users == 4
        and levels < 8
        and pick_tile(local_movies, TILES) is not None
        and pick_tile(local_movies, PARTS) is not None
    )


def reconstruct(hidden_rows, weight_table, bias_row, rated_mask, levels):
    group_rows = hidden_rows.shape[0]
    rating_logits = (
        lax.dot_general(
            hidden_rows, weight_table, (((1,), (1,)), ((), ())), preferred_element_type=jnp.float32
        )
        + bias_row[None, :]
    )
    shaped = rating_logits.reshape(group_rows, levels, -1)
    largest = jnp.max(shaped, axis=1, keepdims=True)
    exponent = jnp.exp(shaped - largest)
    softened = (exponent / jnp.sum(exponent, axis=1, keepdims=True)).astype(jnp.bfloat16)
    return (softened * rated_mask[:, None, :]).reshape(group_rows, -1)


def hidden_phase(visible, weight_table, hid_bias, local_users, device_index):
    combined = jnp.dot(visible, weight_table, preferred_element_type=jnp.float32)
    all_probs = jax.nn.sigmoid(hid_bias[None, :] + lax.psum(combined, "movie"))
    own_rows = lax.dynamic_slice_in_dim(all_probs, device_index * local_users, local_users, 0)
    return (own_rows, all_probs.astype(jnp.bfloat16))


def on_device(movie_ids, ratings, valid, weights, vis_bias, hid_bias):
    owners = lax.axis_size("movie")
    device_index = lax.axis_index("movie")
    local_users, slot_count = movie_ids.shape
    levels, local_movies, hidden = weights.shape
    columns = levels * local_movies
    group_rows = owners * local_users
    capacity = max(2, 3 * local_users * slot_count // owners)
    flat_ids = movie_ids.reshape(-1)
    owner_ids = flat_ids // local_movies
    column_ids = ratings.reshape(-1) * local_movies + flat_ids % local_movies
    user_ids = jnp.arange(local_users * slot_count, dtype=jnp.int32) // slot_count
    usable = valid.reshape(-1) == 1
    matches = (owner_ids[:, None] == jnp.arange(owners, dtype=jnp.int32)[None, :]) & usable[:, None]
    ranking = jnp.cumsum(matches.astype(jnp.int32), axis=0) - 1
    placed = jnp.sum(jnp.where(matches, ranking, 0), axis=1)
    target = jnp.where(usable, owner_ids, owners)
    user_slots = (
        jnp.zeros((owners, capacity), jnp.int32).at[target, placed].set(user_ids, mode="drop")
    )
    column_slots = (
        jnp.full((owners, capacity), -1, jnp.int32).at[target, placed].set(column_ids, mode="drop")
    )
    got_users, got_columns = (
        lax.all_to_all(user_slots, "movie", split_axis=0, concat_axis=0, tiled=True),
        lax.all_to_all(column_slots, "movie", split_axis=0, concat_axis=0, tiled=True),
    )
    user_hot = (got_users[:, :, None] == jnp.arange(local_users, dtype=jnp.int32)).astype(
        jnp.bfloat16
    )
    column_hot = (got_columns[:, :, None] == jnp.arange(columns, dtype=jnp.int32)).astype(
        jnp.bfloat16
    )
    shown = jnp.einsum("ncu,ncj->nuj", user_hot, column_hot, preferred_element_type=jnp.float32)
    shown = shown.reshape(group_rows, columns).astype(jnp.bfloat16)
    rated_mask = jnp.sum(shown.reshape(group_rows, levels, local_movies), axis=1)
    weight_table = weights.reshape(columns, hidden)
    positive_own, positive_group = hidden_phase(
        shown, weight_table, hid_bias, local_users, device_index
    )
    reconstructed_ratings = reconstruct(
        positive_group, weight_table, vis_bias.reshape(columns), rated_mask, levels
    )
    negative_own, negative_group = hidden_phase(
        reconstructed_ratings, weight_table, hid_bias, local_users, device_index
    )
    contract = (((0,), (0,)), ((), ()))
    weight_grad = lax.dot_general(
        shown, positive_group, contract, preferred_element_type=jnp.float32
    )
    weight_grad = weight_grad - lax.dot_general(
        reconstructed_ratings, negative_group, contract, preferred_element_type=jnp.float32
    )
    visible_grad = jnp.sum(shown.astype(jnp.float32), axis=0) - jnp.sum(
        reconstructed_ratings.astype(jnp.float32), axis=0
    )
    weight_grad, visible_grad = lax.psum((weight_grad, visible_grad), "user")
    hidden_grad = lax.psum(jnp.sum(positive_own - negative_own, axis=0), ("movie", "user"))
    return (
        weight_grad.reshape(levels, local_movies, hidden),
        visible_grad.reshape(levels, local_movies),
        hidden_grad,
        positive_own,
    )


def solution(mesh):
    in_specs = (
        P(("movie", "user"), None),
        P(("movie", "user"), None),
        P(("movie", "user"), None),
        P(None, "movie", None),
        P(None, "movie"),
        P(),
    )
    out_specs = (P(None, "movie", None), P(None, "movie"), P(), P(("movie", "user"), None))

    def step(movie_ids, ratings, valid, weights, vis_bias, hid_bias):
        owners = mesh.shape["movie"]
        local_users = movie_ids.shape[0] // (owners * mesh.shape["user"])
        levels, movies, hidden = weights.shape
        fits = fits_kernels(mesh, local_users, movie_ids.shape[1], levels, movies // owners, hidden)
        return jax.shard_map(
            on_device_kernels if fits else on_device,
            mesh=mesh,
            in_specs=in_specs,
            out_specs=out_specs,
            check_vma=False,
        )(movie_ids, ratings, valid, weights, vis_bias, hid_bias)

    return step
```
